32 devices in a mesh: gx: 4 (over x, core), gy: 8 (over z, y).
Axes of the slice: x: 2, y: 2, z: 4, core: 2. Of those that a mesh axis runs over, the one named last changes fastest.
Arguments:
- state: float32 [256, 2, 128, 128], P(('gx', 'gy')), may hold values from -6 to 6
- hamiltonian: float32 [2, 128, 128], replicated, may hold values from -0.5 to 0.5
- couplings: float32 [16, 128, 128], replicated, may hold values from -0.125 to 0.125
- bath_coef: float32 [2, 16], replicated, may hold values from 0.2 to 1
- bath_rate: float32 [16], replicated, may hold values from 0.02 to 0.2
- occupation: int32 [256, 16], P(('gx', 'gy')), may hold values from 0 to 5
- send_list: int32 [32, 32, 1], P(('gx', 'gy')), may hold values from -1 to 7
- up_index: int32 [256, 16], P(('gx', 'gy')), may hold values from -1 to 39
- down_index: int32 [256, 16], P(('gx', 'gy')), may hold values from -1 to 39
- step: float32 [1], replicated, may hold values from 0.5 to 1.5
Outputs:
- derivative: float32 [256, 2, 128, 128], P(('gx', 'gy'))
- advanced: float32 [256, 2, 128, 128], P(('gx', 'gy'))
The draws below stay inside these ranges and needn't reach their ends.
All inputs are finite; a program needn't handle non-finite values.
Results may differ from the reference program's by a relative error of at most 0.0003.
Values sent between devices are 32-bit elements; how exact they have to be, the bound alone decides.
A program may use at most 256 MiB of HBM per device.

```python
import math
import jax
import jax.numpy as jnp
from jax import lax

NS = 128
K = 16
M_DEV = 8
S = 1
TOTAL = 256


def draw_occupation(key, part):
    devices = TOTAL // M_DEV
    owner = jnp.arange(TOTAL, dtype=jnp.int32) // M_DEV
    highest = jnp.minimum(1 + 5 * owner // max(devices - 1, 1), 5)
    tops = jnp.broadcast_to((highest + 1)[:, None], (TOTAL, K))
    values = jax.random.randint(jax.random.fold_in(key, 11), (TOTAL, K), 0, 6)
    values = jnp.minimum(values, tops - 1)
    return values.at[TOTAL - 1, 0].set(5).astype(jnp.int32)


def draw_send_list(key, part):
    devices = TOTAL // M_DEV
    values = jax.random.randint(jax.random.fold_in(key, 21), (devices, devices, S), 0, M_DEV)
    keep = jax.random.randint(jax.random.fold_in(key, 22), (devices, devices, S), 0, 10) < 7
    values = jnp.where(keep, values, -1)
    values = values.at[0, 0, 0].set(M_DEV - 1).at[0, 1, 0].set(-1)
    return values.astype(jnp.int32)


def neighbour_draw(key, salt):
    devices = TOTAL // M_DEV
    kind = jax.random.randint(jax.random.fold_in(key, salt), (TOTAL, K), 0, 10)
    local = jax.random.randint(jax.random.fold_in(key, salt + 1), (TOTAL, K), 0, M_DEV)
    remote = M_DEV + jax.random.randint(jax.random.fold_in(key, salt + 2), (TOTAL, K), 0, devices * S)
    values = jnp.where(kind < 1, -1, jnp.where(kind < 5, local, remote))
    values = values.at[0, 0].set(M_DEV + devices * S - 1).at[0, 1].set(-1)
    return values.astype(jnp.int32)


def draw_up_index(key, part):
    return neighbour_draw(key, 31)


def draw_down_index(key, part):
    return neighbour_draw(key, 41)


def steps_of(stream_key, extent, pieces, smallest, high):
    gain = 1.0
    for dim, shards_of in pieces:
        steps = jax.random.uniform(jax.random.fold_in(jax.random.fold_in(stream_key, 6), dim), (shards_of,), jnp.float32, smallest / len(pieces), high / len(pieces))
        gain = gain * jnp.repeat(jnp.exp(steps), extent[dim] // shards_of).reshape((-1,) + (1,) * (len(extent) - 1 - dim))
    return gain


def gaussian(stream_key, extent, spread, bound, pieces=(), kind=jnp.bfloat16):
    gain = steps_of(stream_key, extent, pieces, -0.22, 0.18) if pieces else 1.0
    result = jax.random.normal(stream_key, extent, jnp.float32) * spread * gain
    return jnp.minimum(jnp.maximum(result, -bound), bound).astype(kind)


def setup_inputs(seed: int = 0) -> dict:
    splits = jax.random.split(jax.random.key(seed), 11)
    return {
        "state": gaussian(splits[0], (TOTAL, 2, NS, NS), 1.0, 6.0, ((0, 32),), jnp.float32),
        "hamiltonian": gaussian(splits[1], (2, NS, NS), NS ** -0.5, 0.5, (), jnp.float32),
        "couplings": gaussian(splits[2], (K, NS, NS), (NS * K) ** -0.5, 0.125, (), jnp.float32),
        "bath_coef": jnp.clip(jax.random.uniform(splits[3], (2, K), jnp.float32, 0.2, 1.0), 0.2, 1.0),
        "bath_rate": jnp.clip(jnp.exp(jax.random.uniform(splits[4], (K,), jnp.float32, math.log(0.02), math.log(0.2))), 0.02, 0.2),
        "occupation": draw_occupation(jax.random.fold_in(splits[10], 71), 0),
        "send_list": draw_send_list(jax.random.fold_in(splits[10], 71), 0),
        "up_index": draw_up_index(jax.random.fold_in(splits[10], 71), 0),
        "down_index": draw_down_index(jax.random.fold_in(splits[10], 71), 0),
        "step": jnp.clip(jax.random.uniform(splits[9], (1,), jnp.float32, 0.5, 1.5), 0.5, 1.5),
    }


def left_product(matrix, rows):
    return jnp.einsum('ij,mcjl->mcil', matrix, rows, precision=lax.Precision.HIGHEST)

def right_product(rows, matrix):
    return jnp.einsum('mcij,jl->mcil', rows, matrix, precision=lax.Precision.HIGHEST)

def derive(local, buffer, occupation, up_index, down_index, hamiltonian, couplings, bath_coef, bath_rate):
    counts = occupation.astype(local.dtype)
    modes = couplings.shape[0]
    rows = local.shape[0]
    joined = jnp.concatenate([up_index, down_index], axis=1).T.reshape(-1)
    picked = jnp.take(buffer, jnp.clip(joined, 0, buffer.shape[0] - 1).astype(jnp.int32), axis=0)
    picked = picked * (joined >= 0).astype(buffer.dtype)[:, None, None, None]
    picked = picked.reshape((2 * modes, rows) + local.shape[1:])
    stacked = jnp.concatenate([couplings, couplings], axis=0)
    lefts = jnp.einsum('kij,kmcjl->kmcil', stacked, picked, precision=lax.Precision.HIGHEST)
    rights = jnp.einsum('kmcij,kjl->kmcil', picked, stacked, precision=lax.Precision.HIGHEST)
    comm = lax.optimization_barrier(jnp.sum(lefts[:modes] - rights[:modes], axis=0))
    left_low, right_low = (lefts[modes:], rights[modes:])
    coef_real = bath_coef[0][:, None, None, None]
    coef_imag = bath_coef[1][:, None, None, None]
    part_x = coef_real * (left_low[:, :, 0] - right_low[:, :, 0]) - coef_imag * (left_low[:, :, 1] + right_low[:, :, 1])
    part_y = coef_real * (left_low[:, :, 1] - right_low[:, :, 1]) + coef_imag * (left_low[:, :, 0] + right_low[:, :, 0])
    weight = counts.T[:, :, None, None]
    sum_x = lax.optimization_barrier(jnp.sum(weight * part_x, axis=0))
    sum_y = lax.optimization_barrier(jnp.sum(weight * part_y, axis=0))
    total = jnp.stack([comm[:, 1] + sum_y, -comm[:, 0] - sum_x], axis=1)
    ham_real, ham_imag = (hamiltonian[0], hamiltonian[1])
    real_part, imag_part = (local[:, 0:1], local[:, 1:2])
    left_real = left_product(ham_real, real_part) - left_product(ham_imag, imag_part)
    left_imag = left_product(ham_real, imag_part) + left_product(ham_imag, real_part)
    right_real = right_product(real_part, ham_real) - right_product(imag_part, ham_imag)
    right_imag = right_product(real_part, ham_imag) + right_product(imag_part, ham_real)
    comm_real = left_real - right_real
    comm_imag = left_imag - right_imag
    total = total + jnp.concatenate([comm_imag, -comm_real], axis=1)
    damping = lax.optimization_barrier(jnp.sum(counts * bath_rate[None, :], axis=1))
    return total - damping[:, None, None, None] * local

def reference(state, hamiltonian, couplings, bath_coef, bath_rate, occupation, send_list, up_index, down_index, step):
    devices = TOTAL // M_DEV

    def one_device(dev):
        local = lax.dynamic_slice_in_dim(state, dev * M_DEV, M_DEV, 0)
        chosen = lax.dynamic_index_in_dim(send_list, dev, 1, keepdims=False)
        owners = jnp.arange(devices, dtype=jnp.int32)[:, None]
        flat = owners * M_DEV + jnp.clip(chosen, 0, M_DEV - 1).astype(jnp.int32)
        arrived = jnp.take(state, flat.reshape(-1), axis=0)
        arrived = arrived * (chosen.reshape(-1) >= 0).astype(state.dtype)[:, None, None, None]
        buffer = jnp.concatenate([local, arrived], axis=0)
        occ = lax.dynamic_slice_in_dim(occupation, dev * M_DEV, M_DEV, 0)
        ups = lax.dynamic_slice_in_dim(up_index, dev * M_DEV, M_DEV, 0)
        downs = lax.dynamic_slice_in_dim(down_index, dev * M_DEV, M_DEV, 0)
        return derive(local, buffer, occ, ups, downs, hamiltonian, couplings, bath_coef, bath_rate)
    parts = lax.map(one_device, jnp.arange(devices, dtype=jnp.int32))
    derivative = parts.reshape(state.shape)
    count = TOTAL * 2 * NS * NS
    rms = jnp.sqrt(jnp.sum(derivative * derivative) / count + 1e-06)
    advanced = state + step[0] / rms * derivative
    return (derivative, advanced)
```

```python
import functools

import jax
import jax.numpy as jnp
from jax import lax
from jax.experimental import pallas as pl
from jax.experimental.pallas import tpu as pltpu
from jax.sharding import PartitionSpec as P

AXES = ("gx", "gy")
MESH = pl.DeviceIdType.MESH
COMPUTE = True


def split(value):
    high = value.astype(jnp.bfloat16)
    low = (value - high.astype(jnp.float32)).astype(jnp.bfloat16)
    return high, low


def kernel(
    gx, gy, length, strips,
    up, down, occ, coef, rate, step, lists, state, couplings, hamiltonian,
    derivative, advanced,
    own, below, above, arrived, stage, list_v, list_s, from_u, from_w, scale_a, scale_b,
    q_full, q_turned, q_left, q_right, h_full, h_left, h_right, h_x_hi, h_x_lo, h_y,
    x_hi, x_lo, x_hi_2, x_lo_2, y_hi, y_lo, der, adv, squares, gathered,
    load_sem, copy_sem, q_sem, up_sem, down_sem, below_sem, above_sem, list_send, list_recv, list_load, plane_send, plane_recv,
    sum_send, sum_recv, out_sem,
):
    rows, modes = up.shape
    n_size = state.shape[2]
    count = gx * gy
    side = gy // length
    columns = gx * side
    slots = lists.shape[1]
    size = n_size // strips
    x, y = lax.axis_index("gx"), lax.axis_index("gy")
    me = x * gy + y
    z, yy = y // side, lax.rem(y, side)
    column = x * side + yy
    dot = functools.partial(jnp.dot, preferred_element_type=jnp.float32)

    def place(at, level):
        return at // side, level * side + lax.rem(at, side)

    def strip(h):
        return pl.ds(h * size, size)

    barrier = pltpu.get_barrier_semaphore()

    def load(h):
        return pltpu.make_async_copy(state.at[:, :, strip(h)], own[h], load_sem.at[h])

    def load_again(h):
        return pltpu.make_async_copy(state.at[:, :, strip(h)], arrived[h].at[pl.ds(0, rows)], copy_sem.at[h])

    for h in range(strips):
        load(h).start()
    load_list = pltpu.make_async_copy(lists.at[0], list_s.at[z], list_load.at[0])
    load_list.start()

    @pl.loop(1, count)
    def _(hop):
        other = lax.rem(me + hop, count)
        pl.semaphore_signal(barrier, inc=1, device_id=(other // gy, lax.rem(other, gy)), device_id_type=MESH)

    for h in range(strips):
        load_again(h).start()
    load_q = pltpu.make_async_copy(couplings, q_full, q_sem.at[0])
    load_h = pltpu.make_async_copy(hamiltonian, h_full, q_sem.at[1])
    load_q.start()
    load_h.start()
    pl.semaphore_wait(barrier, count - 1)

    def relay(hop, h, way):
        held = below if way > 0 else above
        return pltpu.make_async_remote_copy(
            src_ref=held[hop - 1][h] if hop else own[h],
            dst_ref=held[hop][h],
            send_sem=(up_sem if way > 0 else down_sem).at[hop, h],
            recv_sem=(below_sem if way > 0 else above_sem).at[hop, h],
            device_id=place(column, z + way),
            device_id_type=MESH,
        )

    def send_lists(hop):
        return pltpu.make_async_remote_copy(
            src_ref=lists.at[0],
            dst_ref=list_v.at[z],
            send_sem=list_send.at[hop],
            recv_sem=list_recv.at[hop],
            device_id=place(column, lax.rem(z + hop, length)),
            device_id_type=MESH,
        )

    for hop in range(1, length):
        send_lists(hop).start()
    for h in range(strips):
        load(h).wait()

        @pl.when(z + 1 < length)
        def _():
            relay(0, h, 1).start()

        @pl.when(z > 0)
        def _():
            relay(0, h, -1).start()

    load_list.wait()

    def hand(level, h, hop, slot):
        return pltpu.make_async_remote_copy(
            src_ref=stage.at[level, h, hop * slots + slot],
            dst_ref=arrived[h].at[rows + (level * columns + hop) * slots + slot],
            send_sem=plane_send.at[level, h],
            recv_sem=plane_recv.at[level, h],
            device_id=place(lax.rem(column + hop, columns), z),
            device_id_type=MESH,
        )

    def all_hands(level, h):
        part = pl.ds(slots, (columns - 1) * slots)
        return pltpu.make_async_remote_copy(
            src_ref=stage.at[level, h, part],
            dst_ref=arrived[h].at[pl.ds(rows + (level * columns + 1) * slots, (columns - 1) * slots)],
            send_sem=plane_send.at[level, h],
            recv_sem=plane_recv.at[level, h],
            device_id=place(lax.rem(column + 1, columns), z),
            device_id_type=MESH,
        )

    def chosen(held, level, at, slot):
        target = place(at, z)
        pick = list_s[level, slot, target[0] * gy + target[1]]
        keep = jnp.where(pick < 0, 0.0, 1.0).astype(jnp.float32)
        pick = jnp.clip(pick, 0, rows - 1)
        return held[pick] * keep

    def distribute(held, level, h):
        for slot in range(slots):

            @pl.loop(1, columns)
            def _(hop):
                stage[level, h, hop * slots + slot] = chosen(held, level, lax.rem(column + hop, columns), slot)
                hand(level, h, hop, slot).start()

            arrived[h][rows + level * columns * slots + slot] = chosen(held, level, column, slot)

    for h in range(strips):
        distribute(own[h], z, h)

    def arrive(hop, h):
        low, high = z - hop, z + hop

        @pl.when(low >= 0)
        def _():
            relay(hop - 1, h, 1).wait_recv()
            if hop + 1 < length:

                @pl.when(z + 1 < length)
                def _():
                    relay(hop, h, 1).start()

        @pl.when(high < length)
        def _():
            relay(hop - 1, h, -1).wait_recv()
            if hop + 1 < length:

                @pl.when(z > 0)
                def _():
                    relay(hop, h, -1).start()

        @pl.when(low >= 0)
        def _():
            distribute(below[hop - 1][h], low, h)

        @pl.when(high < length)
        def _():
            distribute(above[hop - 1][h], high, h)

    for hop in range(1, length):
        send_lists(hop).wait()
    for hop in range(1, length):
        level = lax.rem(z + hop, length)
        copy = pltpu.make_async_copy(list_v.at[level], list_s.at[level], list_load.at[hop])
        copy.start()
        copy.wait()

    load_q.wait()
    load_h.wait()
    for k in range(modes):
        high, low = split(q_full[k])
        at = pl.ds(k * n_size, n_size)
        q_right[at, pl.ds(0, n_size)] = high
        q_right[at, pl.ds(n_size, n_size)] = low
        q_turned[k] = q_full[k].T
    for k in range(2):
        high, low = split(h_full[k])
        at = pl.ds(k * n_size, n_size)
        h_right[at, pl.ds(0, n_size)] = high
        h_right[at, pl.ds(n_size, n_size)] = low
        h_left[pl.ds(0, n_size), at] = high
        h_left[pl.ds(n_size, n_size), at] = low

    for h in range(strips):
        arrive(1, h)

    for h in range(strips):
        turned = q_turned[:, h * size:(h + 1) * size, :].reshape(modes * size, n_size).T
        high, low = split(turned)
        q_left[h, pl.ds(0, n_size), :] = high
        q_left[h, pl.ds(n_size, n_size), :] = low

    empty = rows + count * slots

    def position(index):
        source = (index - rows) // slots
        slot = lax.rem(index - rows, slots) if slots > 1 else 0
        sx, sy = source // gy, lax.rem(source, gy)
        hop = lax.rem(column + columns - (sx * side + lax.rem(sy, side)), columns)
        far = rows + ((sy // side) * columns + hop) * slots + slot
        return jnp.where(index < 0, empty, jnp.where(index < rows, index, far))

    @pl.loop(0, rows)
    def _(n):
        for k in range(modes):
            weight = occ[n, k].astype(jnp.float32)
            from_u[n, k] = position(up[n, k])
            from_w[n, k] = position(down[n, k])
            scale_a[n, k] = weight * coef[0, k]
            scale_b[n, k] = weight * coef[1, k]

    for h in range(strips):
        arrived[h][empty] = jnp.zeros((2, size, n_size), jnp.float32)

    @pl.loop(0, rows)
    def _(n):
        for h in range(strips):
            re, im = own[h][n, 0], own[h][n, 1]
            at, at_2 = strip(h), pl.ds(n_size + h * size, size)
            one, two = pl.ds(0, n_size), pl.ds(n_size, n_size)
            re_hi, re_lo = split(re)
            im_hi, im_lo = split(im)
            h_x_hi[at, one], h_x_hi[at, two] = re_hi, im_hi
            h_x_lo[at, one], h_x_lo[at, two] = re_lo, im_lo
            h_x_hi[at_2, one], h_x_hi[at_2, two] = -im_hi, re_hi
            h_x_lo[at_2, one], h_x_lo[at_2, two] = -im_lo, re_lo
            for part, (first, second) in enumerate(((re_hi, -im_hi), (im_hi, re_hi), (re_lo, -im_lo), (im_lo, re_lo))):
                at_y = pl.ds(part * n_size + h * size, size)
                h_y[at_y, one], h_y[at_y, two] = first, second
        both = dot(h_left[...], h_x_hi[...])
        left = both[:n_size] + both[n_size:] + dot(h_left[:n_size, :], h_x_lo[...])
        right = dot(h_y[...], h_right[...])
        two = 2 * n_size
        right = right[:two, :n_size] + right[:two, n_size:] + right[two:, :n_size]
        damping = jnp.float32(0)
        for k in range(modes):
            damping += occ[n, k].astype(jnp.float32) * rate[k]
        re, im = left[:, :n_size] - right[:n_size], left[:, n_size:] - right[n_size:]
        for h in range(strips):
            at = slice(h * size, (h + 1) * size)
            der[n, 0, strip(h)] = im[at] - damping * own[h][n, 0]
            der[n, 1, strip(h)] = -re[at] - damping * own[h][n, 1]

    for hop in range(2, length - 1):
        for h in range(strips):
            arrive(hop, h)

    def build(h, n, xh, xl):
        source = arrived[h]
        for k in range(modes):
            iu, iw = from_u[n, k], from_w[n, k]
            a, b = scale_a[n, k], scale_b[n, k]
            ur, ui = source[iu, 0], source[iu, 1]
            wr, wi = source[iw, 0], source[iw, 1]
            p, q = ur + a * wr, b * wi
            r, s = ui + a * wi, b * wr
            at = pl.ds(k * size, size)
            for part, value in enumerate((p - q, r + s)):
                lanes = pl.ds(part * n_size, n_size)
                xh[at, lanes], xl[at, lanes] = split(value)
            for part, value in enumerate((p + q, r - s)):
                at_y = pl.ds(pl.multiple_of((n * 2 + part) * size, size), size)
                lanes = pl.ds(k * n_size, n_size)
                y_hi[at_y, lanes], y_lo[at_y, lanes] = split(value)

    def finish(h, n, xh, xl):
        both = dot(q_left[h], xh[...])
        left = both[:n_size] + both[n_size:] + dot(q_left[h, :n_size, :], xl[...])
        der[n, 0] += left[:, n_size:]
        der[n, 1] -= left[:, :n_size]

    def compute(h):
        build(h, 0, x_hi, x_lo)

        @pl.loop(0, rows // 2)
        def _(pair):
            n = pair * 2
            build(h, n + 1, x_hi_2, x_lo_2)
            finish(h, n, x_hi, x_lo)
            build(h, jnp.minimum(n + 2, rows - 2), x_hi, x_lo)
            finish(h, n + 1, x_hi_2, x_lo_2)

        high = dot(y_hi[...], q_right[...])
        right = high[:, :n_size] + high[:, n_size:] + dot(y_lo[...], q_right[:, :n_size])
        for n in range(rows):
            der[n, 0, strip(h)] -= right[(2 * n + 1) * size:(2 * n + 2) * size]
            der[n, 1, strip(h)] += right[2 * n * size:(2 * n + 1) * size]

    def process(h):
        for level in range(length):
            all_hands(level, h).wait_recv()
        if COMPUTE:
            compute(h)

    for h in range(strips):
        load_again(h).wait()

    last = length - 1
    for h in range(strips):
        arrive(last, h)
        if h:
            process(h - 1)
    process(strips - 1)

    squares[...] = jnp.zeros_like(squares)

    @pl.loop(0, rows)
    def _(n):
        re, im = der[n, 0], der[n, 1]
        total = re * re + im * im
        squares[...] += jnp.sum(total.reshape(n_size // 8, 8, n_size), axis=0)

    def copy_to(hop):
        other = lax.rem(me + hop, count)
        return pltpu.make_async_remote_copy(
            src_ref=squares,
            dst_ref=gathered.at[hop],
            send_sem=sum_send.at[hop],
            recv_sem=sum_recv.at[hop],
            device_id=(other // gy, lax.rem(other, gy)),
            device_id_type=MESH,
        )

    @pl.loop(1, count)
    def _(hop):
        copy_to(hop).start()

    out = pltpu.make_async_copy(der, derivative, out_sem.at[0])
    out.start()
    gathered[0] = squares[...]
    for level in range(length):
        for h in range(strips):
            all_hands(level, h).wait_send()

    for hop in range(length - 1):
        for h in range(strips):

            @pl.when(jnp.logical_and(z >= hop, z + 1 < length))
            def _():
                relay(hop, h, 1).wait_send()

            @pl.when(jnp.logical_and(z + hop < length, z > 0))
            def _():
                relay(hop, h, -1).wait_send()

    @pl.loop(1, count)
    def _(hop):
        copy_to(hop).wait()

    total = jnp.sum(jnp.sum(gathered[...], axis=0), axis=(0, 1), keepdims=True)
    scale = step[0] / jnp.sqrt(total / (rows * count * 2 * n_size * n_size) + 1e-06)

    @pl.loop(0, rows)
    def _(n):
        for part in range(2):
            for h in range(strips):
                adv[n, part, strip(h)] = own[h][n, part] + scale * der[n, part, strip(h)]

    out_2 = pltpu.make_async_copy(adv, advanced, out_sem.at[1])
    out_2.start()
    out.wait()
    out_2.wait()


def smem():
    return pl.BlockSpec(memory_space=pltpu.SMEM)


def hbm():
    return pl.BlockSpec(memory_space=pl.ANY)


def line_length(gx, gy):
    side = max(gx // 2, 1)
    return gy // side if gy % side == 0 else gy


def make_body(gx, gy):
    count = gx * gy
    length = line_length(gx, gy)
    columns = count // length

    def body(state, hamiltonian, couplings, bath_coef, bath_rate, occupation, send_list, up_index, down_index, step):
        rows, parts, n_size, _ = state.shape
        modes = couplings.shape[0]
        slots = send_list.shape[2]
        strips = 8 if n_size % 128 == 0 else 1
        size = n_size // strips
        lists = jnp.swapaxes(send_list, 1, 2)
        f32, bf16, i32 = jnp.float32, jnp.bfloat16, jnp.int32
        vmem, sm, dma = pltpu.VMEM, pltpu.SMEM, pltpu.SemaphoreType.DMA
        piece = vmem((rows, parts, size, n_size), f32)
        held = tuple((piece,) * strips for _ in range(length - 1))
        entries = rows + count * slots + 1
        return pl.pallas_call(
            functools.partial(kernel, gx, gy, length, strips),
            out_shape=(jax.ShapeDtypeStruct(state.shape, f32), jax.ShapeDtypeStruct(state.shape, f32)),
            in_specs=[smem()] * 6 + [hbm()] * 4,
            out_specs=(hbm(), hbm()),
            scratch_shapes=[
                (piece,) * strips,
                held,
                held,
                (vmem((entries, parts, size, n_size), f32),) * strips,
                vmem((length, strips, columns * slots, parts, size, n_size), f32),
                vmem((length, slots, count), i32),
                sm((length, slots, count), i32),
                sm((rows, modes), i32),
                sm((rows, modes), i32),
                sm((rows, modes), f32),
                sm((rows, modes), f32),
                vmem(couplings.shape, f32),
                vmem(couplings.shape, f32),
                vmem((strips, 2 * n_size, modes * size), bf16),
                vmem((modes * n_size, 2 * n_size), bf16),
                vmem(hamiltonian.shape, f32),
                vmem((2 * n_size, 2 * n_size), bf16),
                vmem((2 * n_size, 2 * n_size), bf16),
                vmem((2 * n_size, 2 * n_size), bf16),
                vmem((2 * n_size, 2 * n_size), bf16),
                vmem((4 * n_size, 2 * n_size), bf16),
                vmem((modes * size, 2 * n_size), bf16),
                vmem((modes * size, 2 * n_size), bf16),
                vmem((modes * size, 2 * n_size), bf16),
                vmem((modes * size, 2 * n_size), bf16),
                vmem((rows * 2 * size, modes * n_size), bf16),
                vmem((rows * 2 * size, modes * n_size), bf16),
                vmem(state.shape, f32),
                vmem(state.shape, f32),
                vmem((8, n_size), f32),
                vmem((count, 8, n_size), f32),
                dma((strips,)),
                dma((strips,)),
                dma((2,)),
                dma((length, strips)),
                dma((length, strips)),
                dma((length, strips)),
                dma((length, strips)),
                dma((length,)),
                dma((length,)),
                dma((length,)),
                dma((length, strips)),
                dma((length, strips)),
                dma((count,)),
                dma((count,)),
                dma((2,)),
            ],
            compiler_params=pltpu.CompilerParams(collective_id=0, has_side_effects=True, vmem_limit_bytes=60 << 20),
            name="step",
        )(up_index, down_index, occupation, bath_coef, bath_rate, step, lists, state, couplings, hamiltonian)

    return body


def solution(mesh):
    placed = (
        P(AXES, None, None, None),
        P(),
        P(),
        P(),
        P(),
        P(AXES, None),
        P(AXES, None, None),
        P(AXES, None),
        P(AXES, None),
        P(),
    )
    return jax.shard_map(
        make_body(mesh.shape["gx"], mesh.shape["gy"]),
        mesh=mesh,
        in_specs=placed,
        out_specs=(P(AXES, None, None, None), P(AXES, None, None, None)),
        check_vma=False,
    )
```

```python
import functools

import jax
import jax.numpy as jnp
from jax import lax
from jax.experimental import pallas as pl
from jax.experimental.pallas import tpu as pltpu
from jax.sharding import PartitionSpec as P

AXES = ("gx", "gy")
MESH = pl.DeviceIdType.MESH
COMPUTE = True


def split(value):
    high = value.astype(jnp.bfloat16)
    low = (value - high.astype(jnp.float32)).astype(jnp.bfloat16)
    return high, low


def kernel(
    gx, gy, length, strips,
    up, down, occ, coef, rate, step, lists, state, couplings, hamiltonian,
    negative, factor,
    own, below, above, arrived, stage, list_v, list_s, from_u, from_w, scale_a, scale_b,
    q_full, q_turned, q_left, q_right, h_full, h_left, h_right, h_x_hi, h_x_lo, h_y,
    x_hi, x_lo, x_hi_2, x_lo_2, y_hi, y_lo, der, squares, gathered,
    load_sem, copy_sem, q_sem, up_sem, down_sem, below_sem, above_sem, list_send, list_recv, list_load, plane_send, plane_recv,
    sum_send, sum_recv, out_sem,
):
    rows, modes = up.shape
    n_size = state.shape[2]
    count = gx * gy
    side = gy // length
    columns = gx * side
    slots = lists.shape[1]
    size = n_size // strips
    x, y = lax.axis_index("gx"), lax.axis_index("gy")
    me = x * gy + y
    z, yy = y // side, lax.rem(y, side)
    column = x * side + yy
    dot = functools.partial(jnp.dot, preferred_element_type=jnp.float32)

    def place(at, level):
        return at // side, level * side + lax.rem(at, side)

    def strip(h):
        return pl.ds(h * size, size)

    barrier = pltpu.get_barrier_semaphore()

    def load(h):
        return pltpu.make_async_copy(state.at[:, :, strip(h)], own[h], load_sem.at[h])

    def load_again(h):
        return pltpu.make_async_copy(state.at[:, :, strip(h)], arrived[h].at[pl.ds(0, rows)], copy_sem.at[h])

    for h in range(strips):
        load(h).start()
    load_list = pltpu.make_async_copy(lists.at[0], list_s.at[z], list_load.at[0])
    load_list.start()

    for hop in range(1, length):
        pl.semaphore_signal(barrier, inc=1, device_id=place(column, lax.rem(z + hop, length)), device_id_type=MESH)

    @pl.loop(1, columns)
    def _(hop):
        pl.semaphore_signal(barrier, inc=1, device_id=place(lax.rem(column + hop, columns), z), device_id_type=MESH)

    for h in range(strips):
        load_again(h).start()
    load_q = pltpu.make_async_copy(couplings, q_full, q_sem.at[0])
    load_h = pltpu.make_async_copy(hamiltonian, h_full, q_sem.at[1])
    load_q.start()
    load_h.start()
    pl.semaphore_wait(barrier, length + columns - 2)

    def relay(hop, h, way):
        held = below if way > 0 else above
        return pltpu.make_async_remote_copy(
            src_ref=held[hop - 1][h] if hop else own[h],
            dst_ref=held[hop][h],
            send_sem=(up_sem if way > 0 else down_sem).at[hop, h],
            recv_sem=(below_sem if way > 0 else above_sem).at[hop, h],
            device_id=place(column, z + way),
            device_id_type=MESH,
        )

    def send_lists(hop):
        return pltpu.make_async_remote_copy(
            src_ref=lists.at[0],
            dst_ref=list_v.at[z],
            send_sem=list_send.at[hop],
            recv_sem=list_recv.at[hop],
            device_id=place(column, lax.rem(z + hop, length)),
            device_id_type=MESH,
        )

    for hop in range(1, length):
        send_lists(hop).start()
    for h in range(strips):
        load(h).wait()

        @pl.when(z + 1 < length)
        def _():
            relay(0, h, 1).start()

        @pl.when(z > 0)
        def _():
            relay(0, h, -1).start()

    load_list.wait()

    def hand(level, h, hop, slot):
        return pltpu.make_async_remote_copy(
            src_ref=stage.at[level, h, hop * slots + slot],
            dst_ref=arrived[h].at[rows + (level * columns + hop) * slots + slot],
            send_sem=plane_send.at[level, h],
            recv_sem=plane_recv.at[level, h],
            device_id=place(lax.rem(column + hop, columns), z),
            device_id_type=MESH,
        )

    def all_hands(level, h):
        part = pl.ds(slots, (columns - 1) * slots)
        return pltpu.make_async_remote_copy(
            src_ref=stage.at[level, h, part],
            dst_ref=arrived[h].at[pl.ds(rows + (level * columns + 1) * slots, (columns - 1) * slots)],
            send_sem=plane_send.at[level, h],
            recv_sem=plane_recv.at[level, h],
            device_id=place(lax.rem(column + 1, columns), z),
            device_id_type=MESH,
        )

    def chosen(held, level, at, slot):
        target = place(at, z)
        pick = list_s[level, slot, target[0] * gy + target[1]]
        keep = jnp.where(pick < 0, 0.0, 1.0).astype(jnp.float32)
        pick = jnp.clip(pick, 0, rows - 1)
        return held[pick] * keep

    def distribute(held, level, h):
        for slot in range(slots):

            @pl.loop(1, columns)
            def _(hop):
                stage[level, h, hop * slots + slot] = chosen(held, level, lax.rem(column + hop, columns), slot)
                hand(level, h, hop, slot).start()

            arrived[h][rows + level * columns * slots + slot] = chosen(held, level, column, slot)

    for h in range(strips):
        distribute(own[h], z, h)

    def arrive(hop, h):
        low, high = z - hop, z + hop

        @pl.when(low >= 0)
        def _():
            relay(hop - 1, h, 1).wait_recv()
            if hop + 1 < length:

                @pl.when(z + 1 < length)
                def _():
                    relay(hop, h, 1).start()

        @pl.when(high < length)
        def _():
            relay(hop - 1, h, -1).wait_recv()
            if hop + 1 < length:

                @pl.when(z > 0)
                def _():
                    relay(hop, h, -1).start()

        @pl.when(low >= 0)
        def _():
            distribute(below[hop - 1][h], low, h)

        @pl.when(high < length)
        def _():
            distribute(above[hop - 1][h], high, h)

    for hop in range(1, length):
        send_lists(hop).wait()
    for hop in range(1, length):
        level = lax.rem(z + hop, length)
        copy = pltpu.make_async_copy(list_v.at[level], list_s.at[level], list_load.at[hop])
        copy.start()
        copy.wait()

    load_q.wait()
    load_h.wait()
    for k in range(modes):
        high, low = split(q_full[k])
        at = pl.ds(k * n_size, n_size)
        q_right[at, pl.ds(0, n_size)] = high
        q_right[at, pl.ds(n_size, n_size)] = low
        q_turned[k] = q_full[k].T
    for k in range(2):
        high, low = split(h_full[k])
        at = pl.ds(k * n_size, n_size)
        h_right[at, pl.ds(0, n_size)] = high
        h_right[at, pl.ds(n_size, n_size)] = low
        h_left[pl.ds(0, n_size), at] = high
        h_left[pl.ds(n_size, n_size), at] = low

    for h in range(strips):
        arrive(1, h)

    for h in range(strips):
        turned = q_turned[:, h * size:(h + 1) * size, :].reshape(modes * size, n_size).T
        high, low = split(turned)
        q_left[h, pl.ds(0, n_size), :] = high
        q_left[h, pl.ds(n_size, n_size), :] = low

    empty = rows + count * slots

    def position(index):
        source = (index - rows) // slots
        slot = lax.rem(index - rows, slots) if slots > 1 else 0
        sx, sy = source // gy, lax.rem(source, gy)
        hop = lax.rem(column + columns - (sx * side + lax.rem(sy, side)), columns)
        far = rows + ((sy // side) * columns + hop) * slots + slot
        return jnp.where(index < 0, empty, jnp.where(index < rows, index, far))

    @pl.loop(0, rows)
    def _(n):
        for k in range(modes):
            weight = occ[n, k].astype(jnp.float32)
            from_u[n, k] = position(up[n, k])
            from_w[n, k] = position(down[n, k])
            scale_a[n, k] = weight * coef[0, k]
            scale_b[n, k] = weight * coef[1, k]

    for h in range(strips):
        arrived[h][empty] = jnp.zeros((2, size, n_size), jnp.float32)

    @pl.loop(0, rows)
    def _(n):
        for h in range(strips):
            re, im = own[h][n, 0], own[h][n, 1]
            at, at_2 = strip(h), pl.ds(n_size + h * size, size)
            one, two = pl.ds(0, n_size), pl.ds(n_size, n_size)
            re_hi, re_lo = split(re)
            im_hi, im_lo = split(im)
            h_x_hi[at, one], h_x_hi[at, two] = re_hi, im_hi
            h_x_lo[at, one], h_x_lo[at, two] = re_lo, im_lo
            h_x_hi[at_2, one], h_x_hi[at_2, two] = -im_hi, re_hi
            h_x_lo[at_2, one], h_x_lo[at_2, two] = -im_lo, re_lo
            for part, (first, second) in enumerate(((re_hi, -im_hi), (im_hi, re_hi), (re_lo, -im_lo), (im_lo, re_lo))):
                at_y = pl.ds(part * n_size + h * size, size)
                h_y[at_y, one], h_y[at_y, two] = first, second
        both = dot(h_left[...], h_x_hi[...])
        left = both[:n_size] + both[n_size:] + dot(h_left[:n_size, :], h_x_lo[...])
        right = dot(h_y[...], h_right[...])
        two = 2 * n_size
        right = right[:two, :n_size] + right[:two, n_size:] + right[two:, :n_size]
        damping = jnp.float32(0)
        for k in range(modes):
            damping += occ[n, k].astype(jnp.float32) * rate[k]
        re, im = left[:, :n_size] - right[:n_size], left[:, n_size:] - right[n_size:]
        for h in range(strips):
            at = slice(h * size, (h + 1) * size)
            der[n, 0, strip(h)] = damping * own[h][n, 0] - im[at]
            der[n, 1, strip(h)] = damping * own[h][n, 1] + re[at]

    for hop in range(2, length - 1):
        for h in range(strips):
            arrive(hop, h)

    def build(h, n, xh, xl):
        source = arrived[h]
        for k in range(modes):
            iu, iw = from_u[n, k], from_w[n, k]
            a, b = scale_a[n, k], scale_b[n, k]
            ur, ui = source[iu, 0], source[iu, 1]
            wr, wi = source[iw, 0], source[iw, 1]
            p, q = ur + a * wr, b * wi
            r, s = ui + a * wi, b * wr
            at = pl.ds(k * size, size)
            for part, value in enumerate((p - q, r + s)):
                lanes = pl.ds(part * n_size, n_size)
                xh[at, lanes], xl[at, lanes] = split(value)
            for part, value in enumerate((p + q, r - s)):
                at_y = pl.ds(pl.multiple_of((n * 2 + part) * size, size), size)
                lanes = pl.ds(k * n_size, n_size)
                y_hi[at_y, lanes], y_lo[at_y, lanes] = split(value)

    def finish(h, n, xh, xl):
        both = dot(q_left[h], xh[...])
        left = both[:n_size] + both[n_size:] + dot(q_left[h, :n_size, :], xl[...])
        der[n, 0] -= left[:, n_size:]
        der[n, 1] += left[:, :n_size]

    def compute(h):
        build(h, 0, x_hi, x_lo)

        @pl.loop(0, rows // 2)
        def _(pair):
            n = pair * 2
            build(h, n + 1, x_hi_2, x_lo_2)
            finish(h, n, x_hi, x_lo)
            build(h, jnp.minimum(n + 2, rows - 2), x_hi, x_lo)
            finish(h, n + 1, x_hi_2, x_lo_2)

        high = dot(y_hi[...], q_right[...])
        right = high[:, :n_size] + high[:, n_size:] + dot(y_lo[...], q_right[:, :n_size])
        for n in range(rows):
            der[n, 0, strip(h)] += right[(2 * n + 1) * size:(2 * n + 2) * size]
            der[n, 1, strip(h)] -= right[2 * n * size:(2 * n + 1) * size]

    def process(h):
        for level in range(length):
            all_hands(level, h).wait_recv()
        if COMPUTE:
            compute(h)

    for h in range(strips):
        load_again(h).wait()

    last = length - 1
    for h in range(strips):
        arrive(last, h)
        if h:
            process(h - 1)
    process(strips - 1)

    def square(n, total):
        re, im = der[n, 0], der[n, 1]
        return total + jnp.sum((re * re + im * im).reshape(n_size // 8, 8, n_size), axis=0)

    total = lax.fori_loop(0, rows, square, jnp.zeros((8, n_size), jnp.float32))
    squares[...] = jnp.sum(total, axis=0, keepdims=True)

    def copy_to(hop):
        other = lax.rem(me + hop, count)
        return pltpu.make_async_remote_copy(
            src_ref=squares,
            dst_ref=gathered.at[hop],
            send_sem=sum_send.at[hop],
            recv_sem=sum_recv.at[hop],
            device_id=(other // gy, lax.rem(other, gy)),
            device_id_type=MESH,
        )

    @pl.loop(1, count)
    def _(hop):
        copy_to(hop).start()

    out = pltpu.make_async_copy(der, negative, out_sem.at[0])
    out.start()
    gathered[0] = squares[...]
    for level in range(length):
        for h in range(strips):
            all_hands(level, h).wait_send()

    for hop in range(length - 1):
        for h in range(strips):

            @pl.when(jnp.logical_and(z >= hop, z + 1 < length))
            def _():
                relay(hop, h, 1).wait_send()

            @pl.when(jnp.logical_and(z + hop < length, z > 0))
            def _():
                relay(hop, h, -1).wait_send()

    @pl.loop(1, count)
    def _(hop):
        copy_to(hop).wait()

    total = jnp.sum(jnp.sum(gathered[...], axis=0), axis=(0, 1), keepdims=True)
    scale = step[0] / jnp.sqrt(total / (rows * count * 2 * n_size * n_size) + 1e-06)

    factor[...] = jnp.broadcast_to(scale[0], factor.shape)
    out.wait()


def smem():
    return pl.BlockSpec(memory_space=pltpu.SMEM)


def hbm():
    return pl.BlockSpec(memory_space=pl.ANY)


def line_length(gx, gy):
    side = max(gx // 2, 1)
    return gy // side if gy % side == 0 else gy


def make_body(gx, gy):
    count = gx * gy
    length = line_length(gx, gy)
    columns = count // length

    def body(state, hamiltonian, couplings, bath_coef, bath_rate, occupation, send_list, up_index, down_index, step):
        rows, parts, n_size, _ = state.shape
        modes = couplings.shape[0]
        slots = send_list.shape[2]
        strips = 8 if n_size % 128 == 0 else 1
        size = n_size // strips
        lists = jnp.swapaxes(send_list, 1, 2)
        f32, bf16, i32 = jnp.float32, jnp.bfloat16, jnp.int32
        vmem, sm, dma = pltpu.VMEM, pltpu.SMEM, pltpu.SemaphoreType.DMA
        piece = vmem((rows, parts, size, n_size), f32)
        held = tuple((piece,) * strips for _ in range(length - 1))
        entries = rows + count * slots + 1
        negative, factor = pl.pallas_call(
            functools.partial(kernel, gx, gy, length, strips),
            out_shape=(jax.ShapeDtypeStruct(state.shape, f32), jax.ShapeDtypeStruct((1, n_size), f32)),
            in_specs=[smem()] * 6 + [hbm()] * 4,
            out_specs=(hbm(), pl.BlockSpec(memory_space=vmem)),
            scratch_shapes=[
                (piece,) * strips,
                held,
                held,
                (vmem((entries, parts, size, n_size), f32),) * strips,
                vmem((length, strips, columns * slots, parts, size, n_size), f32),
                vmem((length, slots, count), i32),
                sm((length, slots, count), i32),
                sm((rows, modes), i32),
                sm((rows, modes), i32),
                sm((rows, modes), f32),
                sm((rows, modes), f32),
                vmem(couplings.shape, f32),
                vmem(couplings.shape, f32),
                vmem((strips, 2 * n_size, modes * size), bf16),
                vmem((modes * n_size, 2 * n_size), bf16),
                vmem(hamiltonian.shape, f32),
                vmem((2 * n_size, 2 * n_size), bf16),
                vmem((2 * n_size, 2 * n_size), bf16),
                vmem((2 * n_size, 2 * n_size), bf16),
                vmem((2 * n_size, 2 * n_size), bf16),
                vmem((4 * n_size, 2 * n_size), bf16),
                vmem((modes * size, 2 * n_size), bf16),
                vmem((modes * size, 2 * n_size), bf16),
                vmem((modes * size, 2 * n_size), bf16),
                vmem((modes * size, 2 * n_size), bf16),
                vmem((rows * 2 * size, modes * n_size), bf16),
                vmem((rows * 2 * size, modes * n_size), bf16),
                vmem(state.shape, f32),
                vmem((1, n_size), f32),
                vmem((count, 1, n_size), f32),
                dma((strips,)),
                dma((strips,)),
                dma((2,)),
                dma((length, strips)),
                dma((length, strips)),
                dma((length, strips)),
                dma((length, strips)),
                dma((length,)),
                dma((length,)),
                dma((length,)),
                dma((length, strips)),
                dma((length, strips)),
                dma((count,)),
                dma((count,)),
                dma((1,)),
            ],
            compiler_params=pltpu.CompilerParams(collective_id=0, has_side_effects=True, vmem_limit_bytes=60 << 20),
            name="step",
        )(up_index, down_index, occupation, bath_coef, bath_rate, step, lists, state, couplings, hamiltonian)
        return -negative, state - factor[0, 0] * negative

    return body


def solution(mesh):
    placed = (
        P(AXES, None, None, None),
        P(),
        P(),
        P(),
        P(),
        P(AXES, None),
        P(AXES, None, None),
        P(AXES, None),
        P(AXES, None),
        P(),
    )
    return jax.shard_map(
        make_body(mesh.shape["gx"], mesh.shape["gy"]),
        mesh=mesh,
        in_specs=placed,
        out_specs=(P(AXES, None, None, None), P(AXES, None, None, None)),
        check_vma=False,
    )
```

```python
import functools
import math

import jax
import jax.numpy as jnp
from jax import lax
from jax.experimental import pallas as pl
from jax.experimental.pallas import tpu as pltpu
from jax.sharding import PartitionSpec as P

AXES = ("gx", "gy")
MESH = pl.DeviceIdType.MESH
COMPUTE = True


def split(value):
    high = value.astype(jnp.bfloat16)
    low = (value - high.astype(jnp.float32)).astype(jnp.bfloat16)
    return high, low


def kernel(
    gx, gy, length, strips,
    up_ref, down_ref, occ_ref, coef_ref, rate_ref, step, lists, state, couplings, hamiltonian,
    negative, factor,
    up, down, occ, coef, rate, own, below, above, arrived, stage, list_v, list_s, from_u, from_w, scale_a, scale_b,
    q_full, q_turned, q_left, q_right, h_full, h_left, h_right, h_x_hi, h_x_lo, h_y,
    x_hi, x_lo, x_hi_2, x_lo_2, y_hi, y_lo, der, squares, gathered,
    load_sem, copy_sem, q_sem, up_sem, down_sem, below_sem, above_sem, list_up_send, list_up_recv, list_down_send, list_down_recv, list_load, small_sem, near_sem, plane_send, plane_recv,
    sum_send, sum_recv, out_sem,
):
    rows, modes = up.shape
    n_size = state.shape[2]
    count = gx * gy
    side = gy // length
    columns = gx * side
    slots = lists.shape[1]
    size = n_size // strips
    x, y = lax.axis_index("gx"), lax.axis_index("gy")
    me = x * gy + y
    z, yy = y // side, lax.rem(y, side)
    column = x * side + yy
    dot = functools.partial(jnp.dot, preferred_element_type=jnp.float32)

    def place(at, level):
        return at // side, level * side + lax.rem(at, side)

    def strip(h):
        return pl.ds(h * size, size)

    barrier = pltpu.get_barrier_semaphore()

    def load(h):
        return pltpu.make_async_copy(state.at[:, :, strip(h)], own[h], load_sem.at[h])

    def load_again(h):
        return pltpu.make_async_copy(state.at[:, :, strip(h)], arrived[h].at[pl.ds(0, rows)], copy_sem.at[h])

    for h in range(strips):
        load(h).start()
    load_list = pltpu.make_async_copy(lists.at[0], list_s.at[z], list_load.at[0])
    load_list.start()

    cx, cy = column // side, lax.rem(column, side)
    line_x = [(lax.rem(cx + hop, gx), y) for hop in range(1, gx)]
    line_y = [(x, z * side + lax.rem(yy + hop, side)) for hop in range(1, side)]
    near = line_x + line_y

    def signal(sem, device):
        pl.semaphore_signal(sem, inc=1, device_id=device, device_id_type=MESH)

    for way in (1, -1):

        @pl.when(jnp.logical_and(z + way >= 0, z + way < length))
        def _():
            signal(barrier, place(column, z + way))

    for device in near:
        signal(barrier, device)
    smalls = [
        pltpu.make_async_copy(source, target, small_sem.at[i])
        for i, (source, target) in enumerate(
            ((up_ref, up), (down_ref, down), (occ_ref, occ), (coef_ref, coef), (rate_ref, rate))
        )
    ]
    for copy in smalls:
        copy.start()
    for h in range(strips):
        load_again(h).start()
    load_q = pltpu.make_async_copy(couplings, q_full, q_sem.at[0])
    load_h = pltpu.make_async_copy(hamiltonian, h_full, q_sem.at[1])
    load_q.start()
    load_h.start()
    level_peers = jnp.where(z > 0, 1, 0) + jnp.where(z + 1 < length, 1, 0)
    pl.semaphore_wait(barrier, len(near) + level_peers)

    def relay(hop, h, way):
        held = below if way > 0 else above
        return pltpu.make_async_remote_copy(
            src_ref=held[hop - 1][h] if hop else own[h],
            dst_ref=held[hop][h],
            send_sem=(up_sem if way > 0 else down_sem).at[hop, h],
            recv_sem=(below_sem if way > 0 else above_sem).at[hop, h],
            device_id=place(column, z + way),
            device_id_type=MESH,
        )

    def send_list(hop, way):
        level = z - way * hop
        return pltpu.make_async_remote_copy(
            src_ref=list_v.at[level] if hop else lists.at[0],
            dst_ref=list_v.at[level],
            send_sem=(list_up_send if way > 0 else list_down_send).at[hop],
            recv_sem=(list_up_recv if way > 0 else list_down_recv).at[hop],
            device_id=place(column, z + way),
            device_id_type=MESH,
        )

    def goes(hop, way):
        level = z - way * hop
        return jnp.logical_and(jnp.logical_and(level >= 0, level < length), jnp.logical_and(z + way >= 0, z + way < length))

    for way in (1, -1):

        @pl.when(goes(0, way))
        def _():
            send_list(0, way).start()

    for h in range(strips):
        load(h).wait()

        @pl.when(z + 1 < length)
        def _():
            relay(0, h, 1).start()

        @pl.when(z > 0)
        def _():
            relay(0, h, -1).start()

    for device in near:
        signal(near_sem.at[0], device)
    load_list.wait()
    pl.semaphore_wait(near_sem.at[0], len(near))

    def hand(level, h, hop, slot):
        return pltpu.make_async_remote_copy(
            src_ref=stage.at[level, h, hop * slots + slot],
            dst_ref=arrived[h].at[rows + (level * columns + hop) * slots + slot],
            send_sem=plane_send.at[level, h],
            recv_sem=plane_recv.at[level, h],
            device_id=place(lax.rem(column + hop, columns), z),
            device_id_type=MESH,
        )

    def all_hands(level, h):
        part = pl.ds(slots, (columns - 1) * slots)
        return pltpu.make_async_remote_copy(
            src_ref=stage.at[level, h, part],
            dst_ref=arrived[h].at[pl.ds(rows + (level * columns + 1) * slots, (columns - 1) * slots)],
            send_sem=plane_send.at[level, h],
            recv_sem=plane_recv.at[level, h],
            device_id=place(lax.rem(column + 1, columns), z),
            device_id_type=MESH,
        )

    def chosen(held, level, at, slot):
        target = place(at, z)
        pick = list_s[level, slot, target[0] * gy + target[1]]
        keep = jnp.where(pick < 0, 0.0, 1.0).astype(jnp.float32)
        pick = jnp.clip(pick, 0, rows - 1)
        return held[pick] * keep

    def distribute(held, level, h):
        for slot in range(slots):

            @pl.loop(1, columns)
            def _(hop):
                stage[level, h, hop * slots + slot] = chosen(held, level, lax.rem(column + hop, columns), slot)
                hand(level, h, hop, slot).start()

            arrived[h][rows + level * columns * slots + slot] = chosen(held, level, column, slot)

    for h in range(strips):
        distribute(own[h], z, h)

    def take_list(hop, way):
        level = z - way * hop

        @pl.when(jnp.logical_and(level >= 0, level < length))
        def _():
            copy = pltpu.make_async_remote_copy(
                src_ref=lists.at[0],
                dst_ref=list_v.at[level],
                send_sem=(list_up_send if way > 0 else list_down_send).at[hop - 1],
                recv_sem=(list_up_recv if way > 0 else list_down_recv).at[hop - 1],
                device_id=place(column, z),
                device_id_type=MESH,
            )
            copy.wait_recv()
            if hop + 1 < length:

                @pl.when(goes(hop, way))
                def _():
                    send_list(hop, way).start()

            move = pltpu.make_async_copy(list_v.at[level], list_s.at[level], list_load.at[1])
            move.start()
            move.wait()

    def arrive(hop, h):
        low, high = z - hop, z + hop
        if h == 0:
            take_list(hop, 1)
            take_list(hop, -1)

        @pl.when(low >= 0)
        def _():
            relay(hop - 1, h, 1).wait_recv()
            if hop + 1 < length:

                @pl.when(z + 1 < length)
                def _():
                    relay(hop, h, 1).start()

        @pl.when(high < length)
        def _():
            relay(hop - 1, h, -1).wait_recv()
            if hop + 1 < length:

                @pl.when(z > 0)
                def _():
                    relay(hop, h, -1).start()

        @pl.when(low >= 0)
        def _():
            distribute(below[hop - 1][h], low, h)

        @pl.when(high < length)
        def _():
            distribute(above[hop - 1][h], high, h)

    load_q.wait()
    load_h.wait()
    for copy in smalls:
        copy.wait()
    for k in range(modes):
        high, low = split(q_full[k])
        at = pl.ds(k * n_size, n_size)
        q_right[at, pl.ds(0, n_size)] = high
        q_right[at, pl.ds(n_size, n_size)] = low
        q_turned[k] = q_full[k].T
    for k in range(2):
        high, low = split(h_full[k])
        at = pl.ds(k * n_size, n_size)
        h_right[at, pl.ds(0, n_size)] = high
        h_right[at, pl.ds(n_size, n_size)] = low
        h_left[pl.ds(0, n_size), at] = high
        h_left[pl.ds(n_size, n_size), at] = low

    for h in range(strips):
        arrive(1, h)

    for h in range(strips):
        turned = q_turned[:, h * size:(h + 1) * size, :].reshape(modes * size, n_size).T
        high, low = split(turned)
        q_left[h, pl.ds(0, n_size), :] = high
        q_left[h, pl.ds(n_size, n_size), :] = low

    empty = rows + count * slots

    def position(index):
        source = (index - rows) // slots
        slot = lax.rem(index - rows, slots) if slots > 1 else 0
        sx, sy = source // gy, lax.rem(source, gy)
        hop = lax.rem(column + columns - (sx * side + lax.rem(sy, side)), columns)
        far = rows + ((sy // side) * columns + hop) * slots + slot
        return jnp.where(index < 0, empty, jnp.where(index < rows, index, far))

    @pl.loop(0, rows)
    def _(n):
        for k in range(modes):
            weight = occ[n, k].astype(jnp.float32)
            from_u[n, k] = position(up[n, k])
            from_w[n, k] = position(down[n, k])
            scale_a[n, k] = weight * coef[0, k]
            scale_b[n, k] = weight * coef[1, k]

    for h in range(strips):
        arrived[h][empty] = jnp.zeros((2, size, n_size), jnp.float32)

    @pl.loop(0, rows)
    def _(n):
        for h in range(strips):
            re, im = own[h][n, 0], own[h][n, 1]
            at, at_2 = strip(h), pl.ds(n_size + h * size, size)
            one, two = pl.ds(0, n_size), pl.ds(n_size, n_size)
            re_hi, re_lo = split(re)
            im_hi, im_lo = split(im)
            h_x_hi[at, one], h_x_hi[at, two] = re_hi, im_hi
            h_x_lo[at, one], h_x_lo[at, two] = re_lo, im_lo
            h_x_hi[at_2, one], h_x_hi[at_2, two] = -im_hi, re_hi
            h_x_lo[at_2, one], h_x_lo[at_2, two] = -im_lo, re_lo
            for part, (first, second) in enumerate(((re_hi, -im_hi), (im_hi, re_hi), (re_lo, -im_lo), (im_lo, re_lo))):
                at_y = pl.ds(part * n_size + h * size, size)
                h_y[at_y, one], h_y[at_y, two] = first, second
        both = dot(h_left[...], h_x_hi[...])
        left = both[:n_size] + both[n_size:] + dot(h_left[:n_size, :], h_x_lo[...])
        right = dot(h_y[...], h_right[...])
        two = 2 * n_size
        right = right[:two, :n_size] + right[:two, n_size:] + right[two:, :n_size]
        damping = jnp.float32(0)
        for k in range(modes):
            damping += occ[n, k].astype(jnp.float32) * rate[k]
        re, im = left[:, :n_size] - right[:n_size], left[:, n_size:] - right[n_size:]
        for h in range(strips):
            at = slice(h * size, (h + 1) * size)
            der[n, 0, strip(h)] = damping * own[h][n, 0] - im[at]
            der[n, 1, strip(h)] = damping * own[h][n, 1] + re[at]

    for hop in range(2, length - 1):
        for h in range(strips):
            arrive(hop, h)

    def build(h, n, xh, xl):
        source = arrived[h]
        for k in range(modes):
            iu, iw = from_u[n, k], from_w[n, k]
            a, b = scale_a[n, k], scale_b[n, k]
            ur, ui = source[iu, 0], source[iu, 1]
            wr, wi = source[iw, 0], source[iw, 1]
            p, q = ur + a * wr, b * wi
            r, s = ui + a * wi, b * wr
            at = pl.ds(k * size, size)
            for part, value in enumerate((p - q, r + s)):
                lanes = pl.ds(part * n_size, n_size)
                xh[at, lanes], xl[at, lanes] = split(value)
            for part, value in enumerate((p + q, r - s)):
                at_y = pl.ds(pl.multiple_of((n * 2 + part) * size, size), size)
                lanes = pl.ds(k * n_size, n_size)
                y_hi[at_y, lanes], y_lo[at_y, lanes] = split(value)

    def finish(h, n, xh, xl):
        both = dot(q_left[h], xh[...])
        left = both[:n_size] + both[n_size:] + dot(q_left[h, :n_size, :], xl[...])
        der[n, 0] -= left[:, n_size:]
        der[n, 1] += left[:, :n_size]

    def compute(h):
        build(h, 0, x_hi, x_lo)

        @pl.loop(0, rows // 2)
        def _(pair):
            n = pair * 2
            build(h, n + 1, x_hi_2, x_lo_2)
            finish(h, n, x_hi, x_lo)
            build(h, jnp.minimum(n + 2, rows - 2), x_hi, x_lo)
            finish(h, n + 1, x_hi_2, x_lo_2)

        high = dot(y_hi[...], q_right[...])
        right = high[:, :n_size] + high[:, n_size:] + dot(y_lo[...], q_right[:, :n_size])
        for n in range(rows):
            der[n, 0, strip(h)] += right[(2 * n + 1) * size:(2 * n + 2) * size]
            der[n, 1, strip(h)] -= right[2 * n * size:(2 * n + 1) * size]

    def process(h):
        for level in range(length):
            all_hands(level, h).wait_recv()
        if COMPUTE:
            compute(h)

    for h in range(strips):
        load_again(h).wait()

    last = length - 1
    for h in range(strips):
        arrive(last, h)
        if h:
            process(h - 1)
    process(strips - 1)

    def square(n, total):
        re, im = der[n, 0], der[n, 1]
        return total + jnp.sum((re * re + im * im).reshape(n_size // 8, 8, n_size), axis=0)

    total = lax.fori_loop(0, rows, square, jnp.zeros((8, n_size), jnp.float32))
    squares[...] = jnp.sum(total, axis=0, keepdims=True)

    def copy_to(hop):
        other = lax.rem(me + hop, count)
        return pltpu.make_async_remote_copy(
            src_ref=squares,
            dst_ref=gathered.at[hop],
            send_sem=sum_send.at[hop],
            recv_sem=sum_recv.at[hop],
            device_id=(other // gy, lax.rem(other, gy)),
            device_id_type=MESH,
        )

    @pl.loop(1, count)
    def _(hop):
        copy_to(hop).start()

    out = pltpu.make_async_copy(der, negative, out_sem.at[0])
    out.start()
    gathered[0] = squares[...]
    for level in range(length):
        for h in range(strips):
            all_hands(level, h).wait_send()

    for hop in range(length - 1):
        for way in (1, -1):

            @pl.when(goes(hop, way))
            def _():
                send_list(hop, way).wait_send()

        for h in range(strips):

            @pl.when(jnp.logical_and(z >= hop, z + 1 < length))
            def _():
                relay(hop, h, 1).wait_send()

            @pl.when(jnp.logical_and(z + hop < length, z > 0))
            def _():
                relay(hop, h, -1).wait_send()

    @pl.loop(1, count)
    def _(hop):
        copy_to(hop).wait()

    total = jnp.sum(jnp.sum(gathered[...], axis=0), axis=(0, 1), keepdims=True)
    scale = step[0] / jnp.sqrt(total / (rows * count * 2 * n_size * n_size) + 1e-06)

    factor[...] = jnp.broadcast_to(scale[0], factor.shape)
    out.wait()


def hbm(array):
    return pltpu.with_memory_space_constraint(array, pltpu.HBM)


def line_length(gx, gy):
    side = max(gx // 2, 1)
    return gy // side if gy % side == 0 else gy


def make_body(gx, gy):
    count = gx * gy
    length = line_length(gx, gy)
    columns = count // length

    def body(state, hamiltonian, couplings, bath_coef, bath_rate, occupation, send_list, up_index, down_index, step):
        rows, parts, n_size, _ = state.shape
        modes = couplings.shape[0]
        slots = send_list.shape[2]
        strips = 8 if n_size % 128 == 0 else 1
        size = n_size // strips
        lists = jnp.swapaxes(send_list, 1, 2)
        f32, bf16, i32 = jnp.float32, jnp.bfloat16, jnp.int32
        sm, dma = pltpu.SMEM, pltpu.SemaphoreType.DMA
        used = []

        def vmem(shape, dtype, copies=1):
            used.append(math.prod(shape) * jnp.dtype(dtype).itemsize * copies)
            return pltpu.VMEM(shape, dtype)

        def tuple_of(shape, dtype, copies):
            return (vmem(shape, dtype, copies),) * copies

        piece = (rows, parts, size, n_size)
        held = [tuple(tuple_of(piece, f32, strips) for _ in range(length - 1)) for _ in range(2)]
        entries = rows + count * slots + 1
        scratch = [
            sm(up_index.shape, i32),
            sm(down_index.shape, i32),
            sm(occupation.shape, i32),
            sm(bath_coef.shape, f32),
            sm(bath_rate.shape, f32),
            tuple_of(piece, f32, strips),
            *held,
            tuple_of((entries, parts, size, n_size), f32, strips),
            vmem((length, strips, columns * slots, parts, size, n_size), f32),
            vmem((length, slots, count), i32),
            sm((length, slots, count), i32),
            sm((rows, modes), i32),
            sm((rows, modes), i32),
            sm((rows, modes), f32),
            sm((rows, modes), f32),
            vmem(couplings.shape, f32),
            vmem(couplings.shape, f32),
            vmem((strips, 2 * n_size, modes * size), bf16),
            vmem((modes * n_size, 2 * n_size), bf16),
            vmem(hamiltonian.shape, f32),
            vmem((2 * n_size, 2 * n_size), bf16),
            vmem((2 * n_size, 2 * n_size), bf16),
            vmem((2 * n_size, 2 * n_size), bf16),
            vmem((2 * n_size, 2 * n_size), bf16),
            vmem((4 * n_size, 2 * n_size), bf16),
            vmem((modes * size, 2 * n_size), bf16),
            vmem((modes * size, 2 * n_size), bf16),
            vmem((modes * size, 2 * n_size), bf16),
            vmem((modes * size, 2 * n_size), bf16),
            vmem((rows * 2 * size, modes * n_size), bf16),
            vmem((rows * 2 * size, modes * n_size), bf16),
            vmem(state.shape, f32),
            vmem((1, n_size), f32),
            vmem((count, 1, n_size), f32),
            dma((strips,)),
            dma((strips,)),
            dma((2,)),
            dma((length, strips)),
            dma((length, strips)),
            dma((length, strips)),
            dma((length, strips)),
            dma((length,)),
            dma((length,)),
            dma((length,)),
            dma((length,)),
            dma((2,)),
            dma((5,)),
            pltpu.SemaphoreType.REGULAR((1,)),
            dma((length, strips)),
            dma((length, strips)),
            dma((count,)),
            dma((count,)),
            dma((1,)),
        ]
        grant = min(sum(used) + (6 << 20), 60 << 20)
        negative, factor = pl.pallas_call(
            functools.partial(kernel, gx, gy, length, strips),
            out_shape=(jax.ShapeDtypeStruct(state.shape, f32), jax.ShapeDtypeStruct((1, n_size), f32)),
            in_specs=[pl.BlockSpec(memory_space=pltpu.HBM)] * 5 + [pl.BlockSpec(memory_space=pltpu.SMEM)] + [pl.BlockSpec(memory_space=pltpu.HBM)] * 4,
            out_specs=(pl.BlockSpec(memory_space=pl.ANY), pl.BlockSpec(memory_space=pltpu.VMEM)),
            scratch_shapes=scratch,
            compiler_params=pltpu.CompilerParams(collective_id=0, has_side_effects=True, vmem_limit_bytes=grant),
            name="step",
        )(*(hbm(a) for a in (up_index, down_index, occupation, bath_coef, bath_rate)), step, *(hbm(a) for a in (lists, state, couplings, hamiltonian)))
        return -negative, state - factor[0, 0] * negative

    return body


def solution(mesh):
    placed = (
        P(AXES, None, None, None),
        P(),
        P(),
        P(),
        P(),
        P(AXES, None),
        P(AXES, None, None),
        P(AXES, None),
        P(AXES, None),
        P(),
    )
    return jax.shard_map(
        make_body(mesh.shape["gx"], mesh.shape["gy"]),
        mesh=mesh,
        in_specs=placed,
        out_specs=(P(AXES, None, None, None), P(AXES, None, None, None)),
        check_vma=False,
    )
```

```python
import functools
import math

import jax
import jax.numpy as jnp
from jax import lax
from jax.experimental import pallas as pl
from jax.experimental.pallas import tpu as pltpu
from jax.sharding import PartitionSpec as P

AXES = ("gx", "gy")
MESH = pl.DeviceIdType.MESH
COMPUTE = True


def split(value):
    high = value.astype(jnp.bfloat16)
    low = (value - high.astype(jnp.float32)).astype(jnp.bfloat16)
    return high, low


def kernel(
    gx, gy, length, strips,
    up_ref, down_ref, occ_ref, coef_ref, rate_ref, step, lists, state, couplings, hamiltonian,
    negative, factor,
    up, down, occ, coef, rate, own, below, above, arrived, stage, list_v, list_s, from_u, from_w, scale_a, scale_b,
    q_full, q_turned, q_left, q_right, h_full, h_left, h_right, h_x_hi, h_x_lo, h_y,
    sets, der, squares, gathered,
    load_sem, copy_sem, q_sem, up_sem, down_sem, below_sem, above_sem, list_up_send, list_up_recv, list_down_send, list_down_recv, list_load, small_sem, near_sem, plane_send, plane_recv,
    sum_send, sum_recv, out_sem,
):
    rows, modes = up.shape
    n_size = state.shape[2]
    count = gx * gy
    side = gy // length
    columns = gx * side
    slots = lists.shape[1]
    size = n_size // strips
    lane = q_left.shape[3]
    x, y = lax.axis_index("gx"), lax.axis_index("gy")
    me = x * gy + y
    z, yy = y // side, lax.rem(y, side)
    column = x * side + yy
    dot = functools.partial(jnp.dot, preferred_element_type=jnp.float32)

    def place(at, level):
        return at // side, level * side + lax.rem(at, side)

    def strip(h):
        return pl.ds(h * size, size)

    barrier = pltpu.get_barrier_semaphore()

    def load(h):
        return pltpu.make_async_copy(state.at[:, :, strip(h)], own[h], load_sem.at[h])

    def load_again(h):
        return pltpu.make_async_copy(state.at[:, :, strip(h)], arrived[h].at[pl.ds(0, rows)], copy_sem.at[h])

    for h in range(strips):
        load(h).start()
    load_list = pltpu.make_async_copy(lists.at[0], list_s.at[z], list_load.at[0])
    load_list.start()

    cx, cy = column // side, lax.rem(column, side)
    line_x = [(lax.rem(cx + hop, gx), y) for hop in range(1, gx)]
    line_y = [(x, z * side + lax.rem(yy + hop, side)) for hop in range(1, side)]
    near = line_x + line_y

    def signal(sem, device):
        pl.semaphore_signal(sem, inc=1, device_id=device, device_id_type=MESH)

    for way in (1, -1):

        @pl.when(jnp.logical_and(z + way >= 0, z + way < length))
        def _():
            signal(barrier, place(column, z + way))

    for device in near:
        signal(barrier, device)
    smalls = [
        pltpu.make_async_copy(source, target, small_sem.at[i])
        for i, (source, target) in enumerate(
            ((up_ref, up), (down_ref, down), (occ_ref, occ), (coef_ref, coef), (rate_ref, rate))
        )
    ]
    for copy in smalls:
        copy.start()
    for h in range(strips):
        load_again(h).start()
    load_q = pltpu.make_async_copy(couplings, q_full, q_sem.at[0])
    load_h = pltpu.make_async_copy(hamiltonian, h_full, q_sem.at[1])
    load_q.start()
    load_h.start()
    level_peers = jnp.where(z > 0, 1, 0) + jnp.where(z + 1 < length, 1, 0)
    pl.semaphore_wait(barrier, len(near) + level_peers)

    def relay(hop, h, way):
        held = below if way > 0 else above
        return pltpu.make_async_remote_copy(
            src_ref=held[hop - 1][h] if hop else own[h],
            dst_ref=held[hop][h],
            send_sem=(up_sem if way > 0 else down_sem).at[hop, h],
            recv_sem=(below_sem if way > 0 else above_sem).at[hop, h],
            device_id=place(column, z + way),
            device_id_type=MESH,
        )

    def send_list(hop, way):
        level = z - way * hop
        return pltpu.make_async_remote_copy(
            src_ref=list_v.at[level] if hop else lists.at[0],
            dst_ref=list_v.at[level],
            send_sem=(list_up_send if way > 0 else list_down_send).at[hop],
            recv_sem=(list_up_recv if way > 0 else list_down_recv).at[hop],
            device_id=place(column, z + way),
            device_id_type=MESH,
        )

    def goes(hop, way):
        level = z - way * hop
        return jnp.logical_and(jnp.logical_and(level >= 0, level < length), jnp.logical_and(z + way >= 0, z + way < length))

    for way in (1, -1):

        @pl.when(goes(0, way))
        def _():
            send_list(0, way).start()

    for h in range(strips):
        load(h).wait()

        @pl.when(z + 1 < length)
        def _():
            relay(0, h, 1).start()

        @pl.when(z > 0)
        def _():
            relay(0, h, -1).start()

    for device in near:
        signal(near_sem.at[0], device)
    load_list.wait()
    pl.semaphore_wait(near_sem.at[0], len(near))

    def hand(level, h, hop, slot):
        return pltpu.make_async_remote_copy(
            src_ref=stage.at[level, h, hop * slots + slot],
            dst_ref=arrived[h].at[rows + (level * columns + hop) * slots + slot],
            send_sem=plane_send.at[level, h],
            recv_sem=plane_recv.at[level, h],
            device_id=place(lax.rem(column + hop, columns), z),
            device_id_type=MESH,
        )

    def all_hands(level, h):
        part = pl.ds(slots, (columns - 1) * slots)
        return pltpu.make_async_remote_copy(
            src_ref=stage.at[level, h, part],
            dst_ref=arrived[h].at[pl.ds(rows + (level * columns + 1) * slots, (columns - 1) * slots)],
            send_sem=plane_send.at[level, h],
            recv_sem=plane_recv.at[level, h],
            device_id=place(lax.rem(column + 1, columns), z),
            device_id_type=MESH,
        )

    def chosen(held, level, at, slot):
        target = place(at, z)
        pick = list_s[level, slot, target[0] * gy + target[1]]
        keep = jnp.where(pick < 0, 0.0, 1.0).astype(jnp.float32)
        pick = jnp.clip(pick, 0, rows - 1)
        return held[pick] * keep

    def distribute(held, level, h):
        for slot in range(slots):

            @pl.loop(1, columns)
            def _(hop):
                stage[level, h, hop * slots + slot] = chosen(held, level, lax.rem(column + hop, columns), slot)
                hand(level, h, hop, slot).start()

            arrived[h][rows + level * columns * slots + slot] = chosen(held, level, column, slot)

    for h in range(strips):
        distribute(own[h], z, h)

    def take_list(hop, way):
        level = z - way * hop

        @pl.when(jnp.logical_and(level >= 0, level < length))
        def _():
            copy = pltpu.make_async_remote_copy(
                src_ref=lists.at[0],
                dst_ref=list_v.at[level],
                send_sem=(list_up_send if way > 0 else list_down_send).at[hop - 1],
                recv_sem=(list_up_recv if way > 0 else list_down_recv).at[hop - 1],
                device_id=place(column, z),
                device_id_type=MESH,
            )
            copy.wait_recv()
            if hop + 1 < length:

                @pl.when(goes(hop, way))
                def _():
                    send_list(hop, way).start()

            move = pltpu.make_async_copy(list_v.at[level], list_s.at[level], list_load.at[1])
            move.start()
            move.wait()

    def arrive(hop, h):
        low, high = z - hop, z + hop
        if h == 0:
            take_list(hop, 1)
            take_list(hop, -1)

        @pl.when(low >= 0)
        def _():
            relay(hop - 1, h, 1).wait_recv()
            if hop + 1 < length:

                @pl.when(z + 1 < length)
                def _():
                    relay(hop, h, 1).start()

        @pl.when(high < length)
        def _():
            relay(hop - 1, h, -1).wait_recv()
            if hop + 1 < length:

                @pl.when(z > 0)
                def _():
                    relay(hop, h, -1).start()

        @pl.when(low >= 0)
        def _():
            distribute(below[hop - 1][h], low, h)

        @pl.when(high < length)
        def _():
            distribute(above[hop - 1][h], high, h)

    load_q.wait()
    load_h.wait()
    for copy in smalls:
        copy.wait()
    for k in range(modes):
        high, low = split(q_full[k])
        at = pl.ds(k * n_size, n_size)
        q_right[0, at, :] = high
        q_right[1, at, :] = low
        q_turned[k] = q_full[k].T
    for k in range(2):
        high, low = split(h_full[k])
        at = pl.ds(k * n_size, n_size)
        h_right[at, pl.ds(0, n_size)] = high
        h_right[at, pl.ds(n_size, n_size)] = low
        h_left[pl.ds(0, n_size), at] = high
        h_left[pl.ds(n_size, n_size), at] = low

    for h in range(strips):
        arrive(1, h)

    for h in range(strips):
        turned = q_turned[:, h * size:(h + 1) * size, :].reshape(modes * size, n_size).T
        high, low = split(turned)
        for tile in range(q_left.shape[1]):
            lanes = slice(tile * lane, (tile + 1) * lane)
            q_left[h, tile, pl.ds(0, n_size), :] = high[:, lanes]
            q_left[h, tile, pl.ds(n_size, n_size), :] = low[:, lanes]

    empty = rows + count * slots

    def position(index):
        source = (index - rows) // slots
        slot = lax.rem(index - rows, slots) if slots > 1 else 0
        sx, sy = source // gy, lax.rem(source, gy)
        hop = lax.rem(column + columns - (sx * side + lax.rem(sy, side)), columns)
        far = rows + ((sy // side) * columns + hop) * slots + slot
        return jnp.where(index < 0, empty, jnp.where(index < rows, index, far))

    @pl.loop(0, rows)
    def _(n):
        for k in range(modes):
            weight = occ[n, k].astype(jnp.float32)
            from_u[n, k] = position(up[n, k])
            from_w[n, k] = position(down[n, k])
            scale_a[n, k] = weight * coef[0, k]
            scale_b[n, k] = weight * coef[1, k]

    for h in range(strips):
        arrived[h][empty] = jnp.zeros((2, size, n_size), jnp.float32)

    @pl.loop(0, rows)
    def _(n):
        for h in range(strips):
            re, im = own[h][n, 0], own[h][n, 1]
            at, at_2 = strip(h), pl.ds(n_size + h * size, size)
            one, two = pl.ds(0, n_size), pl.ds(n_size, n_size)
            re_hi, re_lo = split(re)
            im_hi, im_lo = split(im)
            h_x_hi[at, one], h_x_hi[at, two] = re_hi, im_hi
            h_x_lo[at, one], h_x_lo[at, two] = re_lo, im_lo
            h_x_hi[at_2, one], h_x_hi[at_2, two] = -im_hi, re_hi
            h_x_lo[at_2, one], h_x_lo[at_2, two] = -im_lo, re_lo
            for part, (first, second) in enumerate(((re_hi, -im_hi), (im_hi, re_hi), (re_lo, -im_lo), (im_lo, re_lo))):
                at_y = pl.ds(part * n_size + h * size, size)
                h_y[at_y, one], h_y[at_y, two] = first, second
        both = dot(h_left[...], h_x_hi[...])
        left = both[:n_size] + both[n_size:] + dot(h_left[:n_size, :], h_x_lo[...])
        right = dot(h_y[...], h_right[...])
        two = 2 * n_size
        right = right[:two, :n_size] + right[:two, n_size:] + right[two:, :n_size]
        damping = jnp.float32(0)
        for k in range(modes):
            damping += occ[n, k].astype(jnp.float32) * rate[k]
        re, im = left[:, :n_size] - right[:n_size], left[:, n_size:] - right[n_size:]
        for h in range(strips):
            at = slice(h * size, (h + 1) * size)
            der[n, 0, strip(h)] = damping * own[h][n, 0] - im[at]
            der[n, 1, strip(h)] = damping * own[h][n, 1] + re[at]

    for hop in range(2, length - 1):
        for h in range(strips):
            arrive(hop, h)

    def build(h, n, place_y, held):
        (xh, xl), y_held = held[0][place_y], held[1]
        source = arrived[h]
        for k in range(modes):
            iu, iw = from_u[n, k], from_w[n, k]
            a, b = scale_a[n, k], scale_b[n, k]
            ur, ui = source[iu, 0], source[iu, 1]
            wr, wi = source[iw, 0], source[iw, 1]
            p, q = ur + a * wr, b * wi
            r, s = ui + a * wi, b * wr
            at = pl.ds(k * size, size)
            for part, value in enumerate((p - q, r + s)):
                xh[part, at, :], xl[part, at, :] = split(value)
            for part, value in enumerate((p + q, r - s)):
                for level, piece in enumerate(split(value)):
                    y_held[k, pl.ds((place_y * 4 + level * 2 + part) * size, size), :] = piece

    def wide(parts):
        return jnp.concatenate(parts, axis=1)

    def finish(h, n, xh, xl):
        matrix = wide([q_left[h, tile] for tile in range(q_left.shape[1])])
        both = dot(matrix, wide([xh[0], xh[1]]))
        left = both[:n_size] + both[n_size:] + dot(matrix[:n_size], wide([xl[0], xl[1]]))
        der[n, 0] -= left[:, n_size:]
        der[n, 1] += left[:, :n_size]

    def finish_right(h, first, held):
        product = dot(wide([held[k] for k in range(modes)]), wide([q_right[0], q_right[1]]))
        for n in range(2):
            re, im, re_lo, im_lo = (product[(4 * n + i) * size:(4 * n + i + 1) * size] for i in range(4))
            der[first + n, 0, strip(h)] += im[:, :n_size] + (im[:, n_size:] + im_lo[:, :n_size])
            der[first + n, 1, strip(h)] -= re[:, :n_size] + (re[:, n_size:] + re_lo[:, :n_size])

    def compute(h):
        for n in range(2):
            build(h, n, n, sets[0])

        def stage(first, held, coming):
            finish_right(h, first, held[1])
            for n in range(2):
                finish(h, first + n, *held[0][n])
            for n in range(2):
                build(h, jnp.minimum(first + 2, rows - 2) + n, n, coming)

        @pl.loop(0, rows // 4)
        def _(four):
            stage(four * 4, sets[0], sets[1])
            stage(four * 4 + 2, sets[1], sets[0])

    def process(h):
        for level in range(length):
            all_hands(level, h).wait_recv()
        if COMPUTE:
            compute(h)

    for h in range(strips):
        load_again(h).wait()

    last = length - 1
    for h in range(strips):
        arrive(last, h)
        if h:
            process(h - 1)
    process(strips - 1)

    def square(n, total):
        re, im = der[n, 0], der[n, 1]
        return total + jnp.sum((re * re + im * im).reshape(n_size // 8, 8, n_size), axis=0)

    total = lax.fori_loop(0, rows, square, jnp.zeros((8, n_size), jnp.float32))
    squares[...] = jnp.sum(total, axis=0, keepdims=True)

    def copy_to(hop):
        other = lax.rem(me + hop, count)
        return pltpu.make_async_remote_copy(
            src_ref=squares,
            dst_ref=gathered.at[hop],
            send_sem=sum_send.at[hop],
            recv_sem=sum_recv.at[hop],
            device_id=(other // gy, lax.rem(other, gy)),
            device_id_type=MESH,
        )

    @pl.loop(1, count)
    def _(hop):
        copy_to(hop).start()

    out = pltpu.make_async_copy(der, negative, out_sem.at[0])
    out.start()
    gathered[0] = squares[...]
    for level in range(length):
        for h in range(strips):
            all_hands(level, h).wait_send()

    for hop in range(length - 1):
        for way in (1, -1):

            @pl.when(goes(hop, way))
            def _():
                send_list(hop, way).wait_send()

        for h in range(strips):

            @pl.when(jnp.logical_and(z >= hop, z + 1 < length))
            def _():
                relay(hop, h, 1).wait_send()

            @pl.when(jnp.logical_and(z + hop < length, z > 0))
            def _():
                relay(hop, h, -1).wait_send()

    @pl.loop(1, count)
    def _(hop):
        copy_to(hop).wait()

    total = jnp.sum(jnp.sum(gathered[...], axis=0), axis=(0, 1), keepdims=True)
    scale = step[0] / jnp.sqrt(total / (rows * count * 2 * n_size * n_size) + 1e-06)

    factor[...] = jnp.broadcast_to(scale[0], factor.shape)
    out.wait()


def hbm(array):
    return pltpu.with_memory_space_constraint(array, pltpu.HBM)


def line_length(gx, gy):
    side = max(gx // 2, 1)
    return gy // side if gy % side == 0 else gy


def make_body(gx, gy):
    count = gx * gy
    length = line_length(gx, gy)
    columns = count // length

    def body(state, hamiltonian, couplings, bath_coef, bath_rate, occupation, send_list, up_index, down_index, step):
        rows, parts, n_size, _ = state.shape
        modes = couplings.shape[0]
        slots = send_list.shape[2]
        strips = 8 if n_size % 128 == 0 else 1
        size = n_size // strips
        lane = math.gcd(modes * size, 128)
        lists = jnp.swapaxes(send_list, 1, 2)
        f32, bf16, i32 = jnp.float32, jnp.bfloat16, jnp.int32
        sm, dma = pltpu.SMEM, pltpu.SemaphoreType.DMA
        used = []

        def vmem(shape, dtype, copies=1):
            used.append(math.prod(shape) * jnp.dtype(dtype).itemsize * copies)
            return pltpu.VMEM(shape, dtype)

        def tuple_of(shape, dtype, copies):
            return (vmem(shape, dtype, copies),) * copies

        piece = (rows, parts, size, n_size)
        held = [tuple(tuple_of(piece, f32, strips) for _ in range(length - 1)) for _ in range(2)]
        entries = rows + count * slots + 1
        scratch = [
            sm(up_index.shape, i32),
            sm(down_index.shape, i32),
            sm(occupation.shape, i32),
            sm(bath_coef.shape, f32),
            sm(bath_rate.shape, f32),
            tuple_of(piece, f32, strips),
            *held,
            tuple_of((entries, parts, size, n_size), f32, strips),
            vmem((length, strips, columns * slots, parts, size, n_size), f32),
            vmem((length, slots, count), i32),
            sm((length, slots, count), i32),
            sm((rows, modes), i32),
            sm((rows, modes), i32),
            sm((rows, modes), f32),
            sm((rows, modes), f32),
            vmem(couplings.shape, f32),
            vmem(couplings.shape, f32),
            vmem((strips, modes * size // lane, 2 * n_size, lane), bf16),
            vmem((2, modes * n_size, n_size), bf16),
            vmem(hamiltonian.shape, f32),
            vmem((2 * n_size, 2 * n_size), bf16),
            vmem((2 * n_size, 2 * n_size), bf16),
            vmem((2 * n_size, 2 * n_size), bf16),
            vmem((2 * n_size, 2 * n_size), bf16),
            vmem((4 * n_size, 2 * n_size), bf16),
            tuple(
                (tuple(tuple_of((2, modes * size, n_size), bf16, 2) for _ in range(2)), vmem((modes, 8 * size, n_size), bf16))
                for _ in range(2)
            ),
            vmem(state.shape, f32),
            vmem((1, n_size), f32),
            vmem((count, 1, n_size), f32),
            dma((strips,)),
            dma((strips,)),
            dma((2,)),
            dma((length, strips)),
            dma((length, strips)),
            dma((length, strips)),
            dma((length, strips)),
            dma((length,)),
            dma((length,)),
            dma((length,)),
            dma((length,)),
            dma((2,)),
            dma((5,)),
            pltpu.SemaphoreType.REGULAR((1,)),
            dma((length, strips)),
            dma((length, strips)),
            dma((count,)),
            dma((count,)),
            dma((1,)),
        ]
        grant = min(sum(used) + (6 << 20), 60 << 20)
        negative, factor = pl.pallas_call(
            functools.partial(kernel, gx, gy, length, strips),
            out_shape=(jax.ShapeDtypeStruct(state.shape, f32), jax.ShapeDtypeStruct((1, n_size), f32)),
            in_specs=[pl.BlockSpec(memory_space=pltpu.HBM)] * 5 + [pl.BlockSpec(memory_space=pltpu.SMEM)] + [pl.BlockSpec(memory_space=pltpu.HBM)] * 4,
            out_specs=(pl.BlockSpec(memory_space=pl.ANY), pl.BlockSpec(memory_space=pltpu.VMEM)),
            scratch_shapes=scratch,
            compiler_params=pltpu.CompilerParams(collective_id=0, has_side_effects=True, vmem_limit_bytes=grant),
            name="step",
        )(*(hbm(a) for a in (up_index, down_index, occupation, bath_coef, bath_rate)), step, *(hbm(a) for a in (lists, state, couplings, hamiltonian)))
        return -negative, state - factor[0, 0] * negative

    return body


def solution(mesh):
    placed = (
        P(AXES, None, None, None),
        P(),
        P(),
        P(),
        P(),
        P(AXES, None),
        P(AXES, None, None),
        P(AXES, None),
        P(AXES, None),
        P(),
    )
    return jax.shard_map(
        make_body(mesh.shape["gx"], mesh.shape["gy"]),
        mesh=mesh,
        in_specs=placed,
        out_specs=(P(AXES, None, None, None), P(AXES, None, None, None)),
        check_vma=False,
    )
```

```python
import functools
import math

import jax
import jax.numpy as jnp
from jax import lax
from jax.experimental import pallas as pl
from jax.experimental.pallas import tpu as pltpu
from jax.sharding import PartitionSpec as P

AXES = ("gx", "gy")
MESH = pl.DeviceIdType.MESH
COMPUTE = True


def split(value):
    high = value.astype(jnp.bfloat16)
    low = (value - high.astype(jnp.float32)).astype(jnp.bfloat16)
    return high, low


def kernel(
    gx, gy, length, strips, direct,
    up_ref, down_ref, occ_ref, coef_ref, rate_ref, step, lists, state, couplings, hamiltonian,
    negative, factor,
    up, down, occ, coef, rate, own, below, above, arrived, stage, list_v, list_s, from_u, from_w, scale_a, scale_b,
    q_full, q_turned, q_left, q_right, h_full, h_left, h_right, h_x_hi, h_x_lo, h_y,
    sets, der, squares, gathered, straight,
    load_sem, copy_sem, q_sem, up_sem, down_sem, below_sem, above_sem, list_up_send, list_up_recv, list_down_send, list_down_recv, list_load, small_sem, near_sem, plane_send, plane_recv,
    sum_send, sum_recv, out_sem, straight_send,
):
    rows, modes = up.shape
    n_size = state.shape[2]
    count = gx * gy
    side = gy // length
    columns = gx * side
    slots = lists.shape[1]
    size = n_size // strips
    lane = q_left.shape[3]
    x, y = lax.axis_index("gx"), lax.axis_index("gy")
    me = x * gy + y
    z, yy = y // side, lax.rem(y, side)
    column = x * side + yy
    dot = functools.partial(jnp.dot, preferred_element_type=jnp.float32)

    last = length - 1

    def place(at, level):
        return at // side, level * side + lax.rem(at, side)

    def strip(h):
        return pl.ds(h * size, size)

    barrier = pltpu.get_barrier_semaphore()

    def load(h):
        return pltpu.make_async_copy(state.at[:, :, strip(h)], own[h], load_sem.at[h])

    def load_again(h):
        return pltpu.make_async_copy(state.at[:, :, strip(h)], arrived[h].at[pl.ds(0, rows)], copy_sem.at[h])

    for h in range(strips):
        load(h).start()
    load_list = pltpu.make_async_copy(lists.at[0], list_s.at[z], list_load.at[0])
    load_list.start()

    cx, cy = column // side, lax.rem(column, side)
    line_x = [(lax.rem(cx + hop, gx), y) for hop in range(1, gx)]
    line_y = [(x, z * side + lax.rem(yy + hop, side)) for hop in range(1, side)]
    near = line_x + line_y

    def signal(sem, device):
        pl.semaphore_signal(sem, inc=1, device_id=device, device_id_type=MESH)

    for way in (1, -1):

        @pl.when(jnp.logical_and(z + way >= 0, z + way < length))
        def _():
            signal(barrier, place(column, z + way))

    for device in near:
        signal(barrier, device)
    smalls = [
        pltpu.make_async_copy(source, target, small_sem.at[i])
        for i, (source, target) in enumerate(
            ((up_ref, up), (down_ref, down), (occ_ref, occ), (coef_ref, coef), (rate_ref, rate))
        )
    ]
    for copy in smalls:
        copy.start()
    for h in range(strips):
        load_again(h).start()
    load_q = pltpu.make_async_copy(couplings, q_full, q_sem.at[0])
    load_h = pltpu.make_async_copy(hamiltonian, h_full, q_sem.at[1])
    load_q.start()
    load_h.start()
    level_peers = jnp.where(z > 0, 1, 0) + jnp.where(z + 1 < length, 1, 0)
    pl.semaphore_wait(barrier, len(near) + level_peers)

    def relay(hop, h, way):
        held = below if way > 0 else above
        return pltpu.make_async_remote_copy(
            src_ref=held[hop - 1][h] if hop else own[h],
            dst_ref=held[hop][h],
            send_sem=(up_sem if way > 0 else down_sem).at[hop, h],
            recv_sem=(below_sem if way > 0 else above_sem).at[hop, h],
            device_id=place(column, z + way),
            device_id_type=MESH,
        )

    def send_list(hop, way):
        level = z - way * hop
        return pltpu.make_async_remote_copy(
            src_ref=list_v.at[level] if hop else lists.at[0],
            dst_ref=list_v.at[level],
            send_sem=(list_up_send if way > 0 else list_down_send).at[hop],
            recv_sem=(list_up_recv if way > 0 else list_down_recv).at[hop],
            device_id=place(column, z + way),
            device_id_type=MESH,
        )

    def goes(hop, way):
        level = z - way * hop
        return jnp.logical_and(jnp.logical_and(level >= 0, level < length), jnp.logical_and(z + way >= 0, z + way < length))

    for way in (1, -1):

        @pl.when(goes(0, way))
        def _():
            send_list(0, way).start()

    for h in range(strips):
        load(h).wait()

        @pl.when(z + 1 < length)
        def _():
            relay(0, h, 1).start()

        @pl.when(z > 0)
        def _():
            relay(0, h, -1).start()

    for device in near:
        signal(near_sem.at[0], device)
    load_list.wait()
    pl.semaphore_wait(near_sem.at[0], len(near))
    for device in near:
        signal(near_sem.at[1], device)

    def hand(level, h, hop, slot):
        return pltpu.make_async_remote_copy(
            src_ref=stage.at[level, h, hop * slots + slot],
            dst_ref=arrived[h].at[rows + (level * columns + hop) * slots + slot],
            send_sem=plane_send.at[level, h],
            recv_sem=plane_recv.at[level, h],
            device_id=place(lax.rem(column + hop, columns), z),
            device_id_type=MESH,
        )

    def all_hands(level, h):
        part = pl.ds(slots, (columns - 1) * slots)
        return pltpu.make_async_remote_copy(
            src_ref=stage.at[level, h, part],
            dst_ref=arrived[h].at[pl.ds(rows + (level * columns + 1) * slots, (columns - 1) * slots)],
            send_sem=plane_send.at[level, h],
            recv_sem=plane_recv.at[level, h],
            device_id=place(lax.rem(column + 1, columns), z),
            device_id_type=MESH,
        )

    def chosen(held, level, at, slot, to=None):
        target = place(at, z if to is None else to)
        pick = list_s[level, slot, target[0] * gy + target[1]]
        keep = jnp.where(pick < 0, 0.0, 1.0).astype(jnp.float32)
        pick = jnp.clip(pick, 0, rows - 1)
        return held[pick] * keep

    def distribute(held, level, h):
        for slot in range(slots):

            @pl.loop(1, columns)
            def _(hop):
                stage[level, h, hop * slots + slot] = chosen(held, level, lax.rem(column + hop, columns), slot)
                hand(level, h, hop, slot).start()

            arrived[h][rows + level * columns * slots + slot] = chosen(held, level, column, slot)

    for h in range(strips):
        distribute(own[h], z, h)

    def send_straight(held, level, h, way):
        for slot in range(slots):

            @pl.loop(0, columns)
            def _(hop):
                at = lax.rem(column + hop, columns)
                straight[h, hop * slots + slot] = chosen(held, level, at, slot, z + way)
                pltpu.make_async_remote_copy(
                    src_ref=straight.at[h, hop * slots + slot],
                    dst_ref=arrived[h].at[rows + (level * columns + hop) * slots + slot],
                    send_sem=straight_send.at[h],
                    recv_sem=plane_recv.at[level, h],
                    device_id=place(at, z + way),
                    device_id_type=MESH,
                ).start()

    def straight_waits(level, h):
        return pltpu.make_async_remote_copy(
            src_ref=straight.at[h],
            dst_ref=arrived[h].at[pl.ds(rows + level * columns * slots, columns * slots)],
            send_sem=straight_send.at[h],
            recv_sem=plane_recv.at[level, h],
            device_id=place(lax.rem(column + 1, columns), z),
            device_id_type=MESH,
        )

    def take_list(hop, way):
        level = z - way * hop

        @pl.when(jnp.logical_and(level >= 0, level < length))
        def _():
            copy = pltpu.make_async_remote_copy(
                src_ref=lists.at[0],
                dst_ref=list_v.at[level],
                send_sem=(list_up_send if way > 0 else list_down_send).at[hop - 1],
                recv_sem=(list_up_recv if way > 0 else list_down_recv).at[hop - 1],
                device_id=place(column, z),
                device_id_type=MESH,
            )
            copy.wait_recv()
            if hop + 1 < length:

                @pl.when(goes(hop, way))
                def _():
                    send_list(hop, way).start()

            move = pltpu.make_async_copy(list_v.at[level], list_s.at[level], list_load.at[1])
            move.start()
            move.wait()

    def arrive(hop, h):
        low, high = z - hop, z + hop
        if h == 0:
            take_list(hop, 1)
            take_list(hop, -1)

        if direct and hop == last:
            return
        ways = ((1, low, below), (-1, high, above))
        for way, level, held in ways:

            @pl.when(jnp.logical_and(level >= 0, level < length))
            def _():
                relay(hop - 1, h, way).wait_recv()
                if hop + 1 < length:

                    @pl.when(goes(hop, way))
                    def _():
                        if direct and hop == last - 1:
                            send_straight(held[hop - 1][h], level, h, way)
                        else:
                            relay(hop, h, way).start()

        for way, level, held in ways:

            @pl.when(jnp.logical_and(level >= 0, level < length))
            def _():
                distribute(held[hop - 1][h], level, h)

    load_q.wait()
    load_h.wait()
    for copy in smalls:
        copy.wait()
    for k in range(modes):
        high, low = split(q_full[k])
        at = pl.ds(k * n_size, n_size)
        q_right[0, at, :] = high
        q_right[1, at, :] = low
        q_turned[k] = q_full[k].T
    for k in range(2):
        high, low = split(h_full[k])
        at = pl.ds(k * n_size, n_size)
        h_right[at, pl.ds(0, n_size)] = high
        h_right[at, pl.ds(n_size, n_size)] = low
        h_left[pl.ds(0, n_size), at] = high
        h_left[pl.ds(n_size, n_size), at] = low

    for h in range(strips):
        arrive(1, h)

    for h in range(strips):
        turned = q_turned[:, h * size:(h + 1) * size, :].reshape(modes * size, n_size).T
        high, low = split(turned)
        for tile in range(q_left.shape[1]):
            lanes = slice(tile * lane, (tile + 1) * lane)
            q_left[h, tile, pl.ds(0, n_size), :] = high[:, lanes]
            q_left[h, tile, pl.ds(n_size, n_size), :] = low[:, lanes]

    empty = rows + count * slots

    def position(index):
        source = (index - rows) // slots
        slot = lax.rem(index - rows, slots) if slots > 1 else 0
        sx, sy = source // gy, lax.rem(source, gy)
        hop = lax.rem(column + columns - (sx * side + lax.rem(sy, side)), columns)
        far = rows + ((sy // side) * columns + hop) * slots + slot
        return jnp.where(index < 0, empty, jnp.where(index < rows, index, far))

    @pl.loop(0, rows)
    def _(n):
        for k in range(modes):
            weight = occ[n, k].astype(jnp.float32)
            from_u[n, k] = position(up[n, k])
            from_w[n, k] = position(down[n, k])
            scale_a[n, k] = weight * coef[0, k]
            scale_b[n, k] = weight * coef[1, k]

    for h in range(strips):
        arrived[h][empty] = jnp.zeros((2, size, n_size), jnp.float32)

    @pl.loop(0, rows)
    def _(n):
        for h in range(strips):
            re, im = own[h][n, 0], own[h][n, 1]
            at, at_2 = strip(h), pl.ds(n_size + h * size, size)
            one, two = pl.ds(0, n_size), pl.ds(n_size, n_size)
            re_hi, re_lo = split(re)
            im_hi, im_lo = split(im)
            h_x_hi[at, one], h_x_hi[at, two] = re_hi, im_hi
            h_x_lo[at, one], h_x_lo[at, two] = re_lo, im_lo
            h_x_hi[at_2, one], h_x_hi[at_2, two] = -im_hi, re_hi
            h_x_lo[at_2, one], h_x_lo[at_2, two] = -im_lo, re_lo
            for part, (first, second) in enumerate(((re_hi, -im_hi), (im_hi, re_hi), (re_lo, -im_lo), (im_lo, re_lo))):
                at_y = pl.ds(part * n_size + h * size, size)
                h_y[at_y, one], h_y[at_y, two] = first, second
        both = dot(h_left[...], h_x_hi[...])
        left = both[:n_size] + both[n_size:] + dot(h_left[:n_size, :], h_x_lo[...])
        right = dot(h_y[...], h_right[...])
        two = 2 * n_size
        right = right[:two, :n_size] + right[:two, n_size:] + right[two:, :n_size]
        damping = jnp.float32(0)
        for k in range(modes):
            damping += occ[n, k].astype(jnp.float32) * rate[k]
        re, im = left[:, :n_size] - right[:n_size], left[:, n_size:] - right[n_size:]
        for h in range(strips):
            at = slice(h * size, (h + 1) * size)
            der[n, 0, strip(h)] = damping * own[h][n, 0] - im[at]
            der[n, 1, strip(h)] = damping * own[h][n, 1] + re[at]

    pl.semaphore_wait(near_sem.at[1], len(near))
    for hop in range(2, length - 1):
        for h in range(strips):
            arrive(hop, h)

    def build(h, n, place_y, held):
        (xh, xl), y_held = held[0][place_y], held[1]
        source = arrived[h]
        for k in range(modes):
            iu, iw = from_u[n, k], from_w[n, k]
            a, b = scale_a[n, k], scale_b[n, k]
            ur, ui = source[iu, 0], source[iu, 1]
            wr, wi = source[iw, 0], source[iw, 1]
            p, q = ur + a * wr, b * wi
            r, s = ui + a * wi, b * wr
            at = pl.ds(k * size, size)
            for part, value in enumerate((p - q, r + s)):
                xh[part, at, :], xl[part, at, :] = split(value)
            for part, value in enumerate((p + q, r - s)):
                for level, piece in enumerate(split(value)):
                    y_held[k, pl.ds((place_y * 4 + level * 2 + part) * size, size), :] = piece

    def wide(parts):
        return jnp.concatenate(parts, axis=1)

    def finish(h, n, xh, xl):
        matrix = wide([q_left[h, tile] for tile in range(q_left.shape[1])])
        both = dot(matrix, wide([xh[0], xh[1]]))
        left = both[:n_size] + both[n_size:] + dot(matrix[:n_size], wide([xl[0], xl[1]]))
        der[n, 0] -= left[:, n_size:]
        der[n, 1] += left[:, :n_size]

    def finish_right(h, first, held):
        product = dot(wide([held[k] for k in range(modes)]), wide([q_right[0], q_right[1]]))
        for n in range(2):
            re, im, re_lo, im_lo = (product[(4 * n + i) * size:(4 * n + i + 1) * size] for i in range(4))
            der[first + n, 0, strip(h)] += im[:, :n_size] + (im[:, n_size:] + im_lo[:, :n_size])
            der[first + n, 1, strip(h)] -= re[:, :n_size] + (re[:, n_size:] + re_lo[:, :n_size])

    def compute(h):
        for n in range(2):
            build(h, n, n, sets[0])

        def stage(first, held, coming):
            finish_right(h, first, held[1])
            for n in range(2):
                finish(h, first + n, *held[0][n])
            for n in range(2):
                build(h, jnp.minimum(first + 2, rows - 2) + n, n, coming)

        @pl.loop(0, rows // 4)
        def _(four):
            stage(four * 4, sets[0], sets[1])
            stage(four * 4 + 2, sets[1], sets[0])

    def process(h):
        for level in range(length):
            if direct and level in (0, last):

                @pl.when(z == last - level)
                def _():
                    straight_waits(level, h).wait_recv()

                @pl.when(z != last - level)
                def _():
                    all_hands(level, h).wait_recv()
            else:
                all_hands(level, h).wait_recv()
        if COMPUTE:
            compute(h)

    for h in range(strips):
        load_again(h).wait()

    for h in range(strips):
        arrive(last, h)
        if h:
            process(h - 1)
    process(strips - 1)

    def square(n, total):
        re, im = der[n, 0], der[n, 1]
        return total + jnp.sum((re * re + im * im).reshape(n_size // 8, 8, n_size), axis=0)

    total = lax.fori_loop(0, rows, square, jnp.zeros((8, n_size), jnp.float32))
    squares[...] = jnp.sum(total, axis=0, keepdims=True)

    def copy_to(hop):
        other = lax.rem(me + hop, count)
        return pltpu.make_async_remote_copy(
            src_ref=squares,
            dst_ref=gathered.at[hop],
            send_sem=sum_send.at[0],
            recv_sem=sum_recv.at[0],
            device_id=(other // gy, lax.rem(other, gy)),
            device_id_type=MESH,
        )

    @pl.loop(1, count)
    def _(hop):
        copy_to(hop).start()

    out = pltpu.make_async_copy(der, negative, out_sem.at[0])
    out.start()
    gathered[0] = squares[...]
    for level in range(length):
        for h in range(strips):
            if direct and level in (0, last):

                @pl.when(z != last - level)
                def _():
                    all_hands(level, h).wait_send()

                @pl.when(z == (last - 1 if level == 0 else 1))
                def _():
                    straight_waits(level, h).wait_send()
            else:
                all_hands(level, h).wait_send()

    for hop in range(length - 1):
        for way in (1, -1):

            @pl.when(goes(hop, way))
            def _():
                send_list(hop, way).wait_send()
                if not (direct and hop == last - 1):
                    for h in range(strips):
                        relay(hop, h, way).wait_send()

    others = pl.ds(1, count - 1)
    sums = pltpu.make_async_remote_copy(
        src_ref=gathered.at[others],
        dst_ref=gathered.at[others],
        send_sem=sum_send.at[0],
        recv_sem=sum_recv.at[0],
        device_id=place(lax.rem(column + 1, columns), z),
        device_id_type=MESH,
    )
    sums.wait_send()
    sums.wait_recv()

    total = jnp.sum(jnp.sum(gathered[...], axis=0), axis=(0, 1), keepdims=True)
    scale = step[0] / jnp.sqrt(total / (rows * count * 2 * n_size * n_size) + 1e-06)

    factor[...] = jnp.broadcast_to(scale[0], factor.shape)
    out.wait()


def hbm(array):
    return pltpu.with_memory_space_constraint(array, pltpu.HBM)


def line_length(gx, gy):
    side = max(gx // 2, 1)
    return gy // side if gy % side == 0 else gy


def make_body(gx, gy):
    count = gx * gy
    length = line_length(gx, gy)
    columns = count // length

    def body(state, hamiltonian, couplings, bath_coef, bath_rate, occupation, send_list, up_index, down_index, step):
        rows, parts, n_size, _ = state.shape
        modes = couplings.shape[0]
        slots = send_list.shape[2]
        strips = 8 if n_size % 128 == 0 else 1
        size = n_size // strips
        lane = math.gcd(modes * size, 128)
        lists = jnp.swapaxes(send_list, 1, 2)
        f32, bf16, i32 = jnp.float32, jnp.bfloat16, jnp.int32
        sm, dma = pltpu.SMEM, pltpu.SemaphoreType.DMA
        used = []

        def vmem(shape, dtype, copies=1):
            used.append(math.prod(shape) * jnp.dtype(dtype).itemsize * copies)
            return pltpu.VMEM(shape, dtype)

        def tuple_of(shape, dtype, copies):
            return (vmem(shape, dtype, copies),) * copies

        piece = (rows, parts, size, n_size)
        held = [tuple(tuple_of(piece, f32, strips) for _ in range(length - 1)) for _ in range(2)]
        entries = rows + count * slots + 1
        direct = length >= 4 and columns * slots <= rows
        few = columns * slots if direct else 1
        scratch = [
            sm(up_index.shape, i32),
            sm(down_index.shape, i32),
            sm(occupation.shape, i32),
            sm(bath_coef.shape, f32),
            sm(bath_rate.shape, f32),
            tuple_of(piece, f32, strips),
            *held,
            tuple_of((entries, parts, size, n_size), f32, strips),
            vmem((length, strips, columns * slots, parts, size, n_size), f32),
            vmem((length, slots, count), i32),
            sm((length, slots, count), i32),
            sm((rows, modes), i32),
            sm((rows, modes), i32),
            sm((rows, modes), f32),
            sm((rows, modes), f32),
            vmem(couplings.shape, f32),
            vmem(couplings.shape, f32),
            vmem((strips, modes * size // lane, 2 * n_size, lane), bf16),
            vmem((2, modes * n_size, n_size), bf16),
            vmem(hamiltonian.shape, f32),
            vmem((2 * n_size, 2 * n_size), bf16),
            vmem((2 * n_size, 2 * n_size), bf16),
            vmem((2 * n_size, 2 * n_size), bf16),
            vmem((2 * n_size, 2 * n_size), bf16),
            vmem((4 * n_size, 2 * n_size), bf16),
            tuple(
                (tuple(tuple_of((2, modes * size, n_size), bf16, 2) for _ in range(2)), vmem((modes, 8 * size, n_size), bf16))
                for _ in range(2)
            ),
            vmem(state.shape, f32),
            vmem((1, n_size), f32),
            vmem((count, 1, n_size), f32),
            vmem((strips, few, parts, size, n_size) if direct else (1, 1, 1, 8, n_size), f32),
            dma((strips,)),
            dma((strips,)),
            dma((2,)),
            dma((length, strips)),
            dma((length, strips)),
            dma((length, strips)),
            dma((length, strips)),
            dma((length,)),
            dma((length,)),
            dma((length,)),
            dma((length,)),
            dma((2,)),
            dma((5,)),
            pltpu.SemaphoreType.REGULAR((2,)),
            dma((length, strips)),
            dma((length, strips)),
            dma((1,)),
            dma((1,)),
            dma((1,)),
            dma((strips,)),
        ]
        grant = min(sum(used) + (6 << 20), 60 << 20)
        negative, factor = pl.pallas_call(
            functools.partial(kernel, gx, gy, length, strips, direct),
            out_shape=(jax.ShapeDtypeStruct(state.shape, f32), jax.ShapeDtypeStruct((1, n_size), f32)),
            in_specs=[pl.BlockSpec(memory_space=pltpu.HBM)] * 5 + [pl.BlockSpec(memory_space=pltpu.SMEM)] + [pl.BlockSpec(memory_space=pltpu.HBM)] * 4,
            out_specs=(pl.BlockSpec(memory_space=pl.ANY), pl.BlockSpec(memory_space=pltpu.VMEM)),
            scratch_shapes=scratch,
            compiler_params=pltpu.CompilerParams(collective_id=0, has_side_effects=True, vmem_limit_bytes=grant),
            name="step",
        )(*(hbm(a) for a in (up_index, down_index, occupation, bath_coef, bath_rate)), step, *(hbm(a) for a in (lists, state, couplings, hamiltonian)))
        return -negative, state - factor[0, 0] * negative

    return body


def solution(mesh):
    placed = (
        P(AXES, None, None, None),
        P(),
        P(),
        P(),
        P(),
        P(AXES, None),
        P(AXES, None, None),
        P(AXES, None),
        P(AXES, None),
        P(),
    )
    return jax.shard_map(
        make_body(mesh.shape["gx"], mesh.shape["gy"]),
        mesh=mesh,
        in_specs=placed,
        out_specs=(P(AXES, None, None, None), P(AXES, None, None, None)),
        check_vma=False,
    )
```

```python
import functools
import math

import jax
import jax.numpy as jnp
from jax import lax
from jax.experimental import pallas as pl
from jax.experimental.pallas import tpu as pltpu
from jax.sharding import PartitionSpec as P

AXES = ("gx", "gy")
MESH = pl.DeviceIdType.MESH
COMPUTE = True


def split(value):
    high = value.astype(jnp.bfloat16)
    low = (value - high.astype(jnp.float32)).astype(jnp.bfloat16)
    return high, low


def kernel(
    gx, gy, length, strips, direct,
    up_ref, down_ref, occ_ref, coef_ref, rate_ref, step, lists, state, couplings, hamiltonian,
    negative, factor,
    up, down, occ, coef, rate, own, below, above, arrived, stage, list_v, list_s, from_u, from_w, scale_a, scale_b,
    q_full, q_turned, q_left, q_right, h_full, h_left, h_right, h_x_hi, h_x_lo, h_y,
    sets, der, squares, gathered, straight, partial,
    load_sem, copy_sem, q_sem, up_sem, down_sem, below_sem, above_sem, list_up_send, list_up_recv, list_down_send, list_down_recv, list_load, small_sem, near_sem, plane_send, plane_recv,
    sum_send, sum_recv, out_sem, straight_send,
):
    rows, modes = up.shape
    n_size = state.shape[2]
    count = gx * gy
    side = gy // length
    columns = gx * side
    slots = lists.shape[1]
    size = n_size // strips
    lane = q_left.shape[3]
    x, y = lax.axis_index("gx"), lax.axis_index("gy")
    me = x * gy + y
    z, yy = y // side, lax.rem(y, side)
    column = x * side + yy
    dot = functools.partial(jnp.dot, preferred_element_type=jnp.float32)

    last = length - 1

    def place(at, level):
        return at // side, level * side + lax.rem(at, side)

    def strip(h):
        return pl.ds(h * size, size)

    barrier = pltpu.get_barrier_semaphore()

    def load(h):
        return pltpu.make_async_copy(state.at[:, :, strip(h)], own[h], load_sem.at[h])

    def load_again(h):
        return pltpu.make_async_copy(state.at[:, :, strip(h)], arrived[h].at[pl.ds(0, rows)], copy_sem.at[h])


    cx, cy = column // side, lax.rem(column, side)
    line_x = [(lax.rem(cx + hop, gx), y) for hop in range(1, gx)]
    line_y = [(x, z * side + lax.rem(yy + hop, side)) for hop in range(1, side)]
    near = line_x + line_y

    def signal(sem, device):
        pl.semaphore_signal(sem, inc=1, device_id=device, device_id_type=MESH)

    for way in (1, -1):

        @pl.when(jnp.logical_and(z + way >= 0, z + way < length))
        def _():
            signal(barrier, place(column, z + way))

    for device in near:
        signal(barrier, device)
    for h in range(strips):
        load(h).start()
    load_list = pltpu.make_async_copy(lists.at[0], list_s.at[z], list_load.at[0])
    load_list.start()
    smalls = [
        pltpu.make_async_copy(source, target, small_sem.at[i])
        for i, (source, target) in enumerate(
            ((up_ref, up), (down_ref, down), (occ_ref, occ), (coef_ref, coef), (rate_ref, rate))
        )
    ]
    for copy in smalls:
        copy.start()
    for h in range(strips):
        load_again(h).start()
    load_q = pltpu.make_async_copy(couplings, q_full, q_sem.at[0])
    load_h = pltpu.make_async_copy(hamiltonian, h_full, q_sem.at[1])
    load_q.start()
    load_h.start()
    level_peers = jnp.where(z > 0, 1, 0) + jnp.where(z + 1 < length, 1, 0)
    pl.semaphore_wait(barrier, len(near) + level_peers)

    def relay(hop, h, way):
        held = below if way > 0 else above
        return pltpu.make_async_remote_copy(
            src_ref=held[hop - 1][h] if hop else own[h],
            dst_ref=held[hop][h],
            send_sem=(up_sem if way > 0 else down_sem).at[hop, h],
            recv_sem=(below_sem if way > 0 else above_sem).at[hop, h],
            device_id=place(column, z + way),
            device_id_type=MESH,
        )

    def send_list(hop, way):
        level = z - way * hop
        return pltpu.make_async_remote_copy(
            src_ref=list_v.at[level] if hop else lists.at[0],
            dst_ref=list_v.at[level],
            send_sem=(list_up_send if way > 0 else list_down_send).at[hop],
            recv_sem=(list_up_recv if way > 0 else list_down_recv).at[hop],
            device_id=place(column, z + way),
            device_id_type=MESH,
        )

    def goes(hop, way):
        level = z - way * hop
        return jnp.logical_and(jnp.logical_and(level >= 0, level < length), jnp.logical_and(z + way >= 0, z + way < length))

    for way in (1, -1):

        @pl.when(goes(0, way))
        def _():
            send_list(0, way).start()

    for h in range(strips):
        load(h).wait()

        @pl.when(z + 1 < length)
        def _():
            relay(0, h, 1).start()

        @pl.when(z > 0)
        def _():
            relay(0, h, -1).start()

    for device in near:
        signal(near_sem.at[0], device)
    load_list.wait()
    pl.semaphore_wait(near_sem.at[0], len(near))
    for device in near:
        signal(near_sem.at[1], device)

    def hand(level, h, hop, slot):
        return pltpu.make_async_remote_copy(
            src_ref=stage.at[level, h, hop * slots + slot],
            dst_ref=arrived[h].at[rows + (level * columns + hop) * slots + slot],
            send_sem=plane_send.at[level, h],
            recv_sem=plane_recv.at[level, h],
            device_id=place(lax.rem(column + hop, columns), z),
            device_id_type=MESH,
        )

    def all_hands(level, h):
        part = pl.ds(slots, (columns - 1) * slots)
        return pltpu.make_async_remote_copy(
            src_ref=stage.at[level, h, part],
            dst_ref=arrived[h].at[pl.ds(rows + (level * columns + 1) * slots, (columns - 1) * slots)],
            send_sem=plane_send.at[level, h],
            recv_sem=plane_recv.at[level, h],
            device_id=place(lax.rem(column + 1, columns), z),
            device_id_type=MESH,
        )

    def chosen(held, level, at, slot, to=None):
        target = place(at, z if to is None else to)
        pick = list_s[level, slot, target[0] * gy + target[1]]
        keep = jnp.where(pick < 0, 0.0, 1.0).astype(jnp.float32)
        pick = jnp.clip(pick, 0, rows - 1)
        return held[pick] * keep

    def distribute(held, level, h):
        for slot in range(slots):

            @pl.loop(1, columns)
            def _(hop):
                stage[level, h, hop * slots + slot] = chosen(held, level, lax.rem(column + hop, columns), slot)
                hand(level, h, hop, slot).start()

            arrived[h][rows + level * columns * slots + slot] = chosen(held, level, column, slot)

    for h in range(strips):
        distribute(own[h], z, h)

    def send_straight(held, level, h, way):
        for slot in range(slots):

            @pl.loop(0, columns)
            def _(hop):
                at = lax.rem(column + hop, columns)
                straight[h, hop * slots + slot] = chosen(held, level, at, slot, z + way)
                pltpu.make_async_remote_copy(
                    src_ref=straight.at[h, hop * slots + slot],
                    dst_ref=arrived[h].at[rows + (level * columns + hop) * slots + slot],
                    send_sem=straight_send.at[h],
                    recv_sem=plane_recv.at[level, h],
                    device_id=place(at, z + way),
                    device_id_type=MESH,
                ).start()

    def straight_waits(level, h):
        return pltpu.make_async_remote_copy(
            src_ref=straight.at[h],
            dst_ref=arrived[h].at[pl.ds(rows + level * columns * slots, columns * slots)],
            send_sem=straight_send.at[h],
            recv_sem=plane_recv.at[level, h],
            device_id=place(lax.rem(column + 1, columns), z),
            device_id_type=MESH,
        )

    def take_list(hop, way):
        level = z - way * hop

        @pl.when(jnp.logical_and(level >= 0, level < length))
        def _():
            copy = pltpu.make_async_remote_copy(
                src_ref=lists.at[0],
                dst_ref=list_v.at[level],
                send_sem=(list_up_send if way > 0 else list_down_send).at[hop - 1],
                recv_sem=(list_up_recv if way > 0 else list_down_recv).at[hop - 1],
                device_id=place(column, z),
                device_id_type=MESH,
            )
            copy.wait_recv()
            if hop + 1 < length:

                @pl.when(goes(hop, way))
                def _():
                    send_list(hop, way).start()

            move = pltpu.make_async_copy(list_v.at[level], list_s.at[level], list_load.at[1])
            move.start()
            move.wait()

    def arrive(hop, h):
        low, high = z - hop, z + hop
        if h == 0:
            take_list(hop, 1)
            take_list(hop, -1)

        if direct and hop == last:
            return
        ways = ((1, low, below), (-1, high, above))
        for way, level, held in ways:

            @pl.when(jnp.logical_and(level >= 0, level < length))
            def _():
                relay(hop - 1, h, way).wait_recv()
                if hop + 1 < length:

                    @pl.when(goes(hop, way))
                    def _():
                        if direct and hop == last - 1:
                            send_straight(held[hop - 1][h], level, h, way)
                        else:
                            relay(hop, h, way).start()

        for way, level, held in ways:

            @pl.when(jnp.logical_and(level >= 0, level < length))
            def _():
                distribute(held[hop - 1][h], level, h)

    load_q.wait()
    load_h.wait()
    for copy in smalls:
        copy.wait()
    for k in range(modes):
        high, low = split(q_full[k])
        at = pl.ds(k * n_size, n_size)
        q_right[0, at, :] = high
        q_right[1, at, :] = low
        q_turned[k] = q_full[k].T
    for k in range(2):
        high, low = split(h_full[k])
        at = pl.ds(k * n_size, n_size)
        h_right[at, pl.ds(0, n_size)] = high
        h_right[at, pl.ds(n_size, n_size)] = low
        h_left[pl.ds(0, n_size), at] = high
        h_left[pl.ds(n_size, n_size), at] = low

    for h in range(strips):
        arrive(1, h)

    for h in range(strips):
        turned = q_turned[:, h * size:(h + 1) * size, :].reshape(modes * size, n_size).T
        high, low = split(turned)
        for tile in range(q_left.shape[1]):
            lanes = slice(tile * lane, (tile + 1) * lane)
            q_left[h, tile, pl.ds(0, n_size), :] = high[:, lanes]
            q_left[h, tile, pl.ds(n_size, n_size), :] = low[:, lanes]

    empty = rows + count * slots

    def position(index):
        source = (index - rows) // slots
        slot = lax.rem(index - rows, slots) if slots > 1 else 0
        sx, sy = source // gy, lax.rem(source, gy)
        hop = lax.rem(column + columns - (sx * side + lax.rem(sy, side)), columns)
        far = rows + ((sy // side) * columns + hop) * slots + slot
        return jnp.where(index < 0, empty, jnp.where(index < rows, index, far))

    @pl.loop(0, rows)
    def _(n):
        for k in range(modes):
            weight = occ[n, k].astype(jnp.float32)
            from_u[n, k] = position(up[n, k])
            from_w[n, k] = position(down[n, k])
            scale_a[n, k] = weight * coef[0, k]
            scale_b[n, k] = weight * coef[1, k]

    for h in range(strips):
        arrived[h][empty] = jnp.zeros((2, size, n_size), jnp.float32)

    @pl.loop(0, rows)
    def _(n):
        for h in range(strips):
            re, im = own[h][n, 0], own[h][n, 1]
            at, at_2 = strip(h), pl.ds(n_size + h * size, size)
            one, two = pl.ds(0, n_size), pl.ds(n_size, n_size)
            re_hi, re_lo = split(re)
            im_hi, im_lo = split(im)
            h_x_hi[at, one], h_x_hi[at, two] = re_hi, im_hi
            h_x_lo[at, one], h_x_lo[at, two] = re_lo, im_lo
            h_x_hi[at_2, one], h_x_hi[at_2, two] = -im_hi, re_hi
            h_x_lo[at_2, one], h_x_lo[at_2, two] = -im_lo, re_lo
            for part, (first, second) in enumerate(((re_hi, -im_hi), (im_hi, re_hi), (re_lo, -im_lo), (im_lo, re_lo))):
                at_y = pl.ds(part * n_size + h * size, size)
                h_y[at_y, one], h_y[at_y, two] = first, second
        both = dot(h_left[...], h_x_hi[...])
        left = both[:n_size] + both[n_size:] + dot(h_left[:n_size, :], h_x_lo[...])
        right = dot(h_y[...], h_right[...])
        two = 2 * n_size
        right = right[:two, :n_size] + right[:two, n_size:] + right[two:, :n_size]
        damping = jnp.float32(0)
        for k in range(modes):
            damping += occ[n, k].astype(jnp.float32) * rate[k]
        re, im = left[:, :n_size] - right[:n_size], left[:, n_size:] - right[n_size:]
        for h in range(strips):
            at = slice(h * size, (h + 1) * size)
            der[n, 0, strip(h)] = damping * own[h][n, 0] - im[at]
            der[n, 1, strip(h)] = damping * own[h][n, 1] + re[at]

    pl.semaphore_wait(near_sem.at[1], len(near))
    for hop in range(2, length - 1):
        for h in range(strips):
            arrive(hop, h)

    def build(h, n, place_y, held):
        (xh, xl), y_held = held[0][place_y], held[1]
        source = arrived[h]
        for k in range(modes):
            iu, iw = from_u[n, k], from_w[n, k]
            a, b = scale_a[n, k], scale_b[n, k]
            ur, ui = source[iu, 0], source[iu, 1]
            wr, wi = source[iw, 0], source[iw, 1]
            p, q = ur + a * wr, b * wi
            r, s = ui + a * wi, b * wr
            at = pl.ds(k * size, size)
            for part, value in enumerate((p - q, r + s)):
                xh[part, at, :], xl[part, at, :] = split(value)
            for part, value in enumerate((p + q, r - s)):
                for level, piece in enumerate(split(value)):
                    y_held[k, pl.ds((place_y * 4 + level * 2 + part) * size, size), :] = piece

    def wide(parts):
        return jnp.concatenate(parts, axis=1)

    def finish(h, n, xh, xl):
        matrix = wide([q_left[h, tile] for tile in range(q_left.shape[1])])
        both = dot(matrix, wide([xh[0], xh[1]]))
        left = both[:n_size] + both[n_size:] + dot(matrix[:n_size], wide([xl[0], xl[1]]))
        re, im = der[n, 0] - left[:, n_size:], der[n, 1] + left[:, :n_size]
        der[n, 0] = re
        der[n, 1] = im
        if h == strips - 1:
            partial[...] += jnp.sum((re * re + im * im).reshape(n_size // 8, 8, n_size), axis=0)

    def finish_right(h, first, held):
        product = dot(wide([held[k] for k in range(modes)]), wide([q_right[0], q_right[1]]))
        for n in range(2):
            re, im, re_lo, im_lo = (product[(4 * n + i) * size:(4 * n + i + 1) * size] for i in range(4))
            der[first + n, 0, strip(h)] += im[:, :n_size] + (im[:, n_size:] + im_lo[:, :n_size])
            der[first + n, 1, strip(h)] -= re[:, :n_size] + (re[:, n_size:] + re_lo[:, :n_size])

    def compute(h):
        for n in range(2):
            build(h, n, n, sets[0])

        def stage(first, held, coming):
            finish_right(h, first, held[1])
            for n in range(2):
                finish(h, first + n, *held[0][n])
            if coming is not None:
                for n in range(2):
                    build(h, first + 2 + n, n, coming)

        @pl.loop(0, rows // 4 - 1)
        def _(four):
            stage(four * 4, sets[0], sets[1])
            stage(four * 4 + 2, sets[1], sets[0])

        stage(rows - 4, sets[0], sets[1])
        stage(rows - 2, sets[1], None)

    def process(h):
        for level in range(length):
            if direct and level in (0, last):

                @pl.when(z == last - level)
                def _():
                    straight_waits(level, h).wait_recv()

                @pl.when(z != last - level)
                def _():
                    all_hands(level, h).wait_recv()
            else:
                all_hands(level, h).wait_recv()
        if COMPUTE:
            compute(h)

    partial[...] = jnp.zeros_like(partial)
    for h in range(strips):
        load_again(h).wait()

    for h in range(strips):
        arrive(last, h)
        if h:
            process(h - 1)
    process(strips - 1)

    squares[...] = jnp.sum(partial[...], axis=0, keepdims=True)

    def copy_to(hop, other):
        return pltpu.make_async_remote_copy(
            src_ref=squares,
            dst_ref=gathered.at[hop],
            send_sem=sum_send.at[0],
            recv_sem=sum_recv.at[0],
            device_id=other,
            device_id_type=MESH,
        )

    for i in range(length):
        level = jnp.where(2 * z < length, last - i, i)

        @pl.loop(0, columns)
        def _(step_on):
            other = place(lax.rem(column + columns - 1 - step_on, columns), level)
            hop = lax.rem(other[0] * gy + other[1] - me + count, count)

            @pl.when(hop != 0)
            def _():
                copy_to(hop, other).start()

    out = pltpu.make_async_copy(der, negative, out_sem.at[0])
    out.start()
    gathered[0] = squares[...]
    for level in range(length):
        for h in range(strips):
            if direct and level in (0, last):

                @pl.when(z != last - level)
                def _():
                    all_hands(level, h).wait_send()

                @pl.when(z == (last - 1 if level == 0 else 1))
                def _():
                    straight_waits(level, h).wait_send()
            else:
                all_hands(level, h).wait_send()

    for hop in range(length - 1):
        for way in (1, -1):

            @pl.when(goes(hop, way))
            def _():
                send_list(hop, way).wait_send()
                if not (direct and hop == last - 1):
                    for h in range(strips):
                        relay(hop, h, way).wait_send()

    others = pl.ds(1, count - 1)
    sums = pltpu.make_async_remote_copy(
        src_ref=gathered.at[others],
        dst_ref=gathered.at[others],
        send_sem=sum_send.at[0],
        recv_sem=sum_recv.at[0],
        device_id=place(lax.rem(column + 1, columns), z),
        device_id_type=MESH,
    )
    sums.wait_send()
    sums.wait_recv()

    total = jnp.sum(jnp.sum(gathered[...], axis=0), axis=(0, 1), keepdims=True)
    scale = step[0] / jnp.sqrt(total / (rows * count * 2 * n_size * n_size) + 1e-06)

    factor[...] = jnp.broadcast_to(scale[0], factor.shape)
    out.wait()


def hbm(array):
    return pltpu.with_memory_space_constraint(array, pltpu.HBM)


def line_length(gx, gy):
    side = max(gx // 2, 1)
    return gy // side if gy % side == 0 else gy


def make_body(gx, gy):
    count = gx * gy
    length = line_length(gx, gy)
    columns = count // length

    def body(state, hamiltonian, couplings, bath_coef, bath_rate, occupation, send_list, up_index, down_index, step):
        rows, parts, n_size, _ = state.shape
        modes = couplings.shape[0]
        slots = send_list.shape[2]
        strips = 8 if n_size % 128 == 0 else 1
        size = n_size // strips
        lane = math.gcd(modes * size, 128)
        lists = jnp.swapaxes(send_list, 1, 2)
        f32, bf16, i32 = jnp.float32, jnp.bfloat16, jnp.int32
        sm, dma = pltpu.SMEM, pltpu.SemaphoreType.DMA
        used = []

        def vmem(shape, dtype, copies=1):
            used.append(math.prod(shape) * jnp.dtype(dtype).itemsize * copies)
            return pltpu.VMEM(shape, dtype)

        def tuple_of(shape, dtype, copies):
            return (vmem(shape, dtype, copies),) * copies

        piece = (rows, parts, size, n_size)
        held = [tuple(tuple_of(piece, f32, strips) for _ in range(length - 1)) for _ in range(2)]
        entries = rows + count * slots + 1
        direct = length >= 4 and columns * slots <= rows
        few = columns * slots if direct else 1
        scratch = [
            sm(up_index.shape, i32),
            sm(down_index.shape, i32),
            sm(occupation.shape, i32),
            sm(bath_coef.shape, f32),
            sm(bath_rate.shape, f32),
            tuple_of(piece, f32, strips),
            *held,
            tuple_of((entries, parts, size, n_size), f32, strips),
            vmem((length, strips, columns * slots, parts, size, n_size), f32),
            vmem((length, slots, count), i32),
            sm((length, slots, count), i32),
            sm((rows, modes), i32),
            sm((rows, modes), i32),
            sm((rows, modes), f32),
            sm((rows, modes), f32),
            vmem(couplings.shape, f32),
            vmem(couplings.shape, f32),
            vmem((strips, modes * size // lane, 2 * n_size, lane), bf16),
            vmem((2, modes * n_size, n_size), bf16),
            vmem(hamiltonian.shape, f32),
            vmem((2 * n_size, 2 * n_size), bf16),
            vmem((2 * n_size, 2 * n_size), bf16),
            vmem((2 * n_size, 2 * n_size), bf16),
            vmem((2 * n_size, 2 * n_size), bf16),
            vmem((4 * n_size, 2 * n_size), bf16),
            tuple(
                (tuple(tuple_of((2, modes * size, n_size), bf16, 2) for _ in range(2)), vmem((modes, 8 * size, n_size), bf16))
                for _ in range(2)
            ),
            vmem(state.shape, f32),
            vmem((1, n_size), f32),
            vmem((count, 1, n_size), f32),
            vmem((strips, few, parts, size, n_size) if direct else (1, 1, 1, 8, n_size), f32),
            vmem((8, n_size), f32),
            dma((strips,)),
            dma((strips,)),
            dma((2,)),
            dma((length, strips)),
            dma((length, strips)),
            dma((length, strips)),
            dma((length, strips)),
            dma((length,)),
            dma((length,)),
            dma((length,)),
            dma((length,)),
            dma((2,)),
            dma((5,)),
            pltpu.SemaphoreType.REGULAR((2,)),
            dma((length, strips)),
            dma((length, strips)),
            dma((1,)),
            dma((1,)),
            dma((1,)),
            dma((strips,)),
        ]
        grant = min(sum(used) + (6 << 20), 60 << 20)
        negative, factor = pl.pallas_call(
            functools.partial(kernel, gx, gy, length, strips, direct),
            out_shape=(jax.ShapeDtypeStruct(state.shape, f32), jax.ShapeDtypeStruct((1, n_size), f32)),
            in_specs=[pl.BlockSpec(memory_space=pltpu.HBM)] * 5 + [pl.BlockSpec(memory_space=pltpu.SMEM)] + [pl.BlockSpec(memory_space=pltpu.HBM)] * 4,
            out_specs=(pl.BlockSpec(memory_space=pl.ANY), pl.BlockSpec(memory_space=pltpu.VMEM)),
            scratch_shapes=scratch,
            compiler_params=pltpu.CompilerParams(collective_id=0, has_side_effects=True, vmem_limit_bytes=grant),
            name="step",
        )(*(hbm(a) for a in (up_index, down_index, occupation, bath_coef, bath_rate)), step, *(hbm(a) for a in (lists, state, couplings, hamiltonian)))
        return -negative, state - factor[0, 0] * negative

    return body


def solution(mesh):
    placed = (
        P(AXES, None, None, None),
        P(),
        P(),
        P(),
        P(),
        P(AXES, None),
        P(AXES, None, None),
        P(AXES, None),
        P(AXES, None),
        P(),
    )
    return jax.shard_map(
        make_body(mesh.shape["gx"], mesh.shape["gy"]),
        mesh=mesh,
        in_specs=placed,
        out_specs=(P(AXES, None, None, None), P(AXES, None, None, None)),
        check_vma=False,
    )
```
